512 devices in a mesh: grp: 2 (over y), pulse: 32 (over z), chan: 4 (over x), sub: 2 (over core).
Axes of the slice: x: 4, y: 2, z: 32, core: 2. Of those that a mesh axis runs over, the one named last changes fastest.
The devices are a block of a 4x16x32 slice.
Arguments:
- samples: int32 [2, 32, 512, 4096], P(None, ('grp', 'chan', 'sub'), 'pulse'), parts along dimension 1, may hold values from -2048 to 2047
- replica: float32 [2, 4096], replicated, may hold values from -6 to 6
- window: int32 [32, 2], P(('grp', 'chan', 'sub')), parts along dimension 0, may hold values from 1 to 28, as said below
- thresh: int32 [32, 2], P(('grp', 'chan', 'sub')), parts along dimension 0, may hold values from 2 to 32, as said below
Outputs:
- ratio_map: float32 [32, 512, 4096], P(('grp', 'chan', 'sub'), None, 'pulse'), parts along dimension 0
- detections: float32 [2], P('grp'), parts along dimension 0
The draws below stay inside these ranges and needn't reach their ends.
There are 2 independent parts, one for each index of `grp`. The reference program is written for one: setup_inputs(seed, part) draws one part's arguments, and reference() takes and returns one part's arrays. A program takes and returns all parts, laid end to end along the dimension named above; an argument that names none is the same for every part. Nothing has to cross between parts.
Inputs may be any that keep to these rules, and one draw needn't show every extreme that they name: `window`: column 0 is a channel's guard gates on each side, 1 to 4; column 1 its training gates on each side, 14 to 28; some channel has both at their most. `thresh`: column 0 is a numerator of 8 to 32, column 1 a denominator of 2 to 4.
All inputs are finite; a program needn't handle non-finite values.
Results may differ from the reference program's by a relative error of at most 0.0003.
Values sent between devices are 32-bit elements; how exact they have to be, the bound alone decides.
No kernel may reach another device: no remote copies, remote signals or barrier semaphores. Data moves between devices by JAX's collectives and lax.ppermute only.
A program may use at most 64 MiB of HBM per device.

```python
import jax
import jax.numpy as jnp
from jax import lax

PULSES = 512
RANGE = 4096
GUARD_MAX = 4
TRAIN_MAX = 28
CHANNELS = 16


def draw_window(key, part):
    guard_key, train_key, pick_key = jax.random.split(jax.random.fold_in(key, 11), 3)
    guards = jax.random.randint(guard_key, (CHANNELS,), 1, GUARD_MAX + 1)
    trains = jax.random.randint(train_key, (CHANNELS,), TRAIN_MAX // 2, TRAIN_MAX + 1)
    chosen = jax.random.randint(pick_key, (), 0, CHANNELS)
    is_pick = jnp.arange(CHANNELS) == chosen
    guards = jnp.where(is_pick, GUARD_MAX, guards)
    trains = jnp.where(is_pick, TRAIN_MAX, trains)
    return jnp.stack([guards, trains], axis=1).astype(jnp.int32)


def draw_thresh(key, part):
    num_key, den_key = jax.random.split(jax.random.fold_in(key, 23))
    numerators = jax.random.randint(num_key, (CHANNELS,), 8, 33)
    denominators = jax.random.randint(den_key, (CHANNELS,), 2, 5)
    return jnp.stack([numerators, denominators], axis=1).astype(jnp.int32)


def with_ends(array, rng, least, top_value):
    longest = array.shape.index(max(array.shape))
    spots = []
    for shift in (0, 1):
        where = [jax.random.randint(jax.random.fold_in(rng, axis), (), 0, length) for axis, length in enumerate(array.shape)]
        where[longest] = (where[longest] + shift) % array.shape[longest]
        spots.append(tuple(where))
    return array.at[spots[0]].set(least).at[spots[1]].set(top_value)


def gaussian(key, shape, spread, bound, kind=jnp.bfloat16):
    array = jax.random.normal(key, shape, jnp.float32) * spread
    return jnp.minimum(jnp.maximum(array, -bound), bound).astype(kind)


def setup_inputs(seed: int = 0, part: int = 0) -> dict:
    key_of = jax.random.split(jax.random.key(seed), 5)
    own_keys = jax.random.split(jax.random.fold_in(key_of[4], part), 5)
    samples = with_ends(jax.random.randint(own_keys[0], (2, CHANNELS, PULSES, RANGE), -2048, 2048), jax.random.fold_in(own_keys[0], 1), -2048, 2047).astype(jnp.int32)
    replica = gaussian(key_of[1], (2, RANGE), 1.0, 6.0, jnp.float32)
    window = draw_window(jax.random.fold_in(jax.random.fold_in(key_of[4], part), 71), part)
    thresh = draw_thresh(jax.random.fold_in(jax.random.fold_in(key_of[4], part), 71), part)
    return {"samples": samples, "replica": replica, "window": window, "thresh": thresh}


def reference(samples, replica, window, thresh):
    margin = GUARD_MAX + TRAIN_MAX
    filt = lax.complex(replica[0], replica[1])

    def per_channel(index):
        chan_samples = lax.dynamic_index_in_dim(samples, index, 1, keepdims=False)
        chan_window = lax.dynamic_index_in_dim(window, index, 0, keepdims=False)
        chan_thresh = lax.dynamic_index_in_dim(thresh, index, 0, keepdims=False)
        signal = lax.complex(chan_samples[0].astype(jnp.float32) / 2048.0, chan_samples[1].astype(jnp.float32) / 2048.0)
        spectrum = jnp.fft.fft(signal, axis=-1, norm="ortho")
        compressed = jnp.fft.ifft(spectrum * filt[None, :], axis=-1, norm="ortho")
        doppler = jnp.fft.fft(compressed, axis=0, norm="ortho")
        power = jnp.real(doppler) ** 2 + jnp.imag(doppler) ** 2
        guard = chan_window[0]
        train = chan_window[1]
        padded = jnp.pad(power, ((0, 0), (margin, margin)))
        inside = jnp.pad(jnp.ones((RANGE,), jnp.float32), (margin, margin))
        noise_sum = jnp.zeros_like(power)
        cells = jnp.zeros((RANGE,), jnp.float32)
        for offset in range(1, margin + 1):
            weight = ((offset > guard) & (offset <= guard + train)).astype(jnp.float32)
            noise_sum = noise_sum + weight * (padded[:, margin + offset:margin + offset + RANGE] + padded[:, margin - offset:margin - offset + RANGE])
            cells = cells + weight * (inside[margin + offset:margin + offset + RANGE] + inside[margin - offset:margin - offset + RANGE])
        level = (noise_sum + 1e-6) / cells[None, :]
        ratio = power / level
        scale = chan_thresh[0].astype(jnp.float32) / chan_thresh[1].astype(jnp.float32)
        soft = jnp.clip(ratio / scale - 1.0, 0.0, 1.0)
        return ratio, jnp.sum(soft)

    ratio_map, soft_sums = lax.map(per_channel, jnp.arange(CHANNELS, dtype=jnp.int32))
    detections = jnp.sum(soft_sums) * (1024.0 / (PULSES * RANGE))
    return ratio_map, detections.reshape(1)
```

```python
import functools
import math

import jax
import jax.numpy as jnp
import numpy as np
from jax import lax
from jax.experimental import pallas as pl
from jax.experimental.pallas import tpu as pltpu
from jax.sharding import PartitionSpec as P

PULSES = 512
RANGE = 4096
GUARD_MAX = 4
TRAIN_MAX = 28

EPSILON = 1e-06
INPUT_SCALE = 1.0 / 2048.0
MARGIN = GUARD_MAX + TRAIN_MAX

LANES = 128
ROWS = 8
FAN = 32
TAIL = RANGE // FAN
FINE = PULSES // FAN
PARTS = MARGIN
PACK = LANES // PARTS
F32 = jnp.float32
BF16 = jnp.bfloat16
MEBI = 1 << 20
ORDER = [place ^ (place >> 1) for place in range(FAN)]


def slot(device):
    return ORDER.index(device)


def split_table(table):
    high = table.astype(BF16)
    low = (table - high.astype(np.float64)).astype(BF16)
    return np.stack([high, low])


def unit(product, period):
    angle = 2.0 * np.pi / period * (np.asarray(product, np.int64) % period)
    return np.cos(angle), np.sin(angle)


def range_tables():
    b = np.arange(TAIL)[:, None]
    col = np.arange(TAIL)[None, :]
    freq = 4 * (col % FAN) + col // FAN
    cos, sin = unit(b * freq, TAIL)
    forward = np.block([[cos, -sin], [sin, cos]])
    inverse = forward.T
    k1 = np.arange(FAN)[:, None]
    cos, sin = unit(k1 * np.arange(TAIL)[None, :], RANGE)
    twiddle = np.stack([cos, sin]).astype(np.float32)
    return split_table(forward), split_table(inverse), twiddle


def doppler_tables():
    tiles = []
    for t in range(FAN // ROWS):
        table = np.zeros((2, FINE, ROWS, ROWS, 2, FINE))
        for d1 in range(ROWS):
            bins = 8 * t + d1 + FAN * np.arange(FINE)[:, None]
            cos, sin = unit(bins * np.arange(FINE)[None, :], PULSES)
            table[0, :, d1, d1, 0] = cos
            table[0, :, d1, d1, 1] = sin
            table[1, :, d1, d1, 0] = -sin
            table[1, :, d1, d1, 1] = cos
        tiles.append(split_table(table.reshape(2 * PULSES // 4, 2 * PULSES // 4)))
    return np.stack(tiles)


def add(x, y):
    return (x[0] + y[0], x[1] + y[1])


def sub(x, y):
    return (x[0] - y[0], x[1] - y[1])


def turn(x, sign):
    return (-x[1], x[0]) if sign > 0 else (x[1], -x[0])


def add_turn(x, y, sign):
    if sign > 0:
        return (x[0] - y[1], x[1] + y[0])
    return (x[0] + y[1], x[1] - y[0])


def by_constant(x, index, period, sign):
    index = index % period
    if index == 0:
        return x
    angle = 2.0 * math.pi * index / period
    cos, sin = math.cos(angle), sign * math.sin(angle)
    if 8 * index == period:
        return ((x[0] - x[1]) * cos, (x[0] + x[1]) * cos) if sign > 0 else ((x[0] + x[1]) * cos, (x[1] - x[0]) * cos)
    if 4 * index == period:
        return turn(x, sign)
    return (x[0] * cos - x[1] * sin, x[0] * sin + x[1] * cos)


def fft4(x, sign):
    a, b = add(x[0], x[2]), sub(x[0], x[2])
    c, d = add(x[1], x[3]), sub(x[1], x[3])
    return [add(a, c), add_turn(b, d, sign), sub(a, c), add_turn(b, d, -sign)]


def fft8(x, sign):
    even, odd = fft4(x[0::2], sign), fft4(x[1::2], sign)
    root = math.sqrt(0.5)
    out = [None] * 8
    out[0], out[4] = add(even[0], odd[0]), sub(even[0], odd[0])
    out[2], out[6] = add_turn(even[2], odd[2], sign), add_turn(even[2], odd[2], -sign)
    for k in (1, 3):
        o = odd[k]
        if k == 1:
            w = (o[0] - o[1], o[0] + o[1]) if sign > 0 else (o[0] + o[1], o[1] - o[0])
        else:
            w = (-o[0] - o[1], o[0] - o[1]) if sign > 0 else (o[1] - o[0], -o[0] - o[1])
        w = (w[0] * root, w[1] * root)
        out[k], out[k + 4] = add(even[k], w), sub(even[k], w)
    return out


def fft32(load, keep, fetch, store, sign):
    for n2 in range(8):
        mid = fft4([load(n2 + 8 * n1) for n1 in range(4)], sign)
        for k1 in range(4):
            keep(k1 * 8 + n2, by_constant(mid[k1], n2 * k1, 32, sign))
    for k1 in range(4):
        out = fft8([fetch(k1 * 8 + n2) for n2 in range(8)], sign)
        for k2 in range(8):
            store(k1 + 4 * k2, out[k2])


def split(x):
    high = x.astype(BF16)
    return high, (x - high.astype(F32)).astype(BF16)


def dot(x, y):
    return jnp.dot(x, y, preferred_element_type=F32)


def compress_kernel(
    x_hbm, rep_hbm, fwd_hbm, inv_hbm, twd_hbm, o_ref,
    x_ref, rep_ref, fwd_ref, inv_ref, twd_ref, h_ref, mid_ref, high_ref, low_ref, sems,
):
    channels, pulses = x_hbm.shape[1], x_hbm.shape[2]
    sets = [(c, p) for c in range(channels) for p in range(0, pulses, ROWS)]
    loads = [
        pltpu.make_async_copy(x_hbm.at[:, c, pl.ds(p, ROWS)], x_ref.at[i], sems.at[i]) for i, (c, p) in enumerate(sets)
    ]
    n = len(sets)
    load_rep = pltpu.make_async_copy(rep_hbm, rep_ref, sems.at[n])
    load_twd = pltpu.make_async_copy(twd_hbm, twd_ref, sems.at[n + 1])
    load_fwd = pltpu.make_async_copy(fwd_hbm, fwd_ref, sems.at[n + 2])
    load_inv = pltpu.make_async_copy(inv_hbm, inv_ref, sems.at[n + 3])
    for load in [loads[0], load_rep, load_twd, load_fwd, *loads[1:], load_inv]:
        load.start()

    load_rep.wait()
    for part in range(2):
        turned = rep_ref[pl.ds(part, FAN, stride=2), :].T
        h_ref[part] = jnp.concatenate([turned[q * FAN : (q + 1) * FAN] for q in range(4)], axis=1)
    load_twd.wait()

    def row(ref, part, k):
        return jnp.broadcast_to(ref[part, k : k + 1, :], (ROWS, LANES))

    def put(i, k, value):
        for part in range(2):
            high, low = split(value[part])
            high_ref[i, k * ROWS : (k + 1) * ROWS, part * LANES : (part + 1) * LANES] = high
            low_ref[i, k * ROWS : (k + 1) * ROWS, part * LANES : (part + 1) * LANES] = low

    def product(i, table):
        high = high_ref[i]
        return dot(high, table[0]) + dot(low_ref[i], table[0]) + dot(high, table[1])

    for i, (c, p) in enumerate(sets):
        loads[i].wait()

        def load(a, i=i):
            return tuple(x_ref[i, part, :, a * LANES : (a + 1) * LANES].astype(F32) for part in range(2))

        def keep(j, value, i=i):
            mid_ref[i, 0, j], mid_ref[i, 1, j] = value

        def fetch(j, i=i):
            return (mid_ref[i, 0, j], mid_ref[i, 1, j])

        def twisted(k, value, i=i):
            cos, sin = row(twd_ref, 0, k) , row(twd_ref, 1, k)
            put(i, k, (value[0] * cos + value[1] * sin, value[1] * cos - value[0] * sin))

        fft32(load, keep, fetch, twisted, -1)
        if i == 0:
            load_fwd.wait()
        spectrum = product(i, fwd_ref)
        for k in range(FAN):
            re = spectrum[k * ROWS : (k + 1) * ROWS, :LANES]
            im = spectrum[k * ROWS : (k + 1) * ROWS, LANES:]
            h_re, h_im = row(h_ref, 0, k), row(h_ref, 1, k)
            put(i, k, (re * h_re - im * h_im, re * h_im + im * h_re))
        if i == 0:
            load_inv.wait()
        back = product(i, inv_ref)

        def untwisted(k, back=back):
            re = back[k * ROWS : (k + 1) * ROWS, :LANES]
            im = back[k * ROWS : (k + 1) * ROWS, LANES:]
            cos, sin = row(twd_ref, 0, k), row(twd_ref, 1, k)
            return (re * cos - im * sin, im * cos + re * sin)

        def store(a, value, i=i):
            for part in range(2):
                o_ref[slot(a), i * 2 * ROWS + part * ROWS : i * 2 * ROWS + (part + 1) * ROWS, :] = value[part]

        fft32(untwisted, keep, fetch, store, 1)


def compress(samples, replica, limit):
    fwd, inv, twd = [jnp.asarray(table) for table in range_tables()]
    sets = samples.shape[1] * samples.shape[2] // ROWS
    rep = replica.reshape(2, FAN, LANES).transpose(1, 0, 2).reshape(2 * FAN, LANES)
    any_space = pl.BlockSpec(memory_space=pltpu.HBM)
    return pl.pallas_call(
        compress_kernel,
        out_shape=pltpu.VMEM((FAN, sets * 2 * ROWS, LANES), F32),
        in_specs=[any_space] * 5,
        out_specs=pl.BlockSpec(memory_space=pltpu.VMEM),
        scratch_shapes=[
            pltpu.VMEM((sets, 2, ROWS, RANGE), jnp.int32),
            pltpu.VMEM((2 * FAN, LANES), F32),
            pltpu.VMEM((2, 2 * TAIL, 2 * TAIL), BF16),
            pltpu.VMEM((2, 2 * TAIL, 2 * TAIL), BF16),
            pltpu.VMEM((2, FAN, LANES), F32),
            pltpu.VMEM((2, FAN, LANES), F32),
            pltpu.VMEM((sets, 2, FAN, ROWS, LANES), F32),
            pltpu.VMEM((sets, FAN * ROWS, 2 * LANES), BF16),
            pltpu.VMEM((sets, FAN * ROWS, 2 * LANES), BF16),
            pltpu.SemaphoreType.DMA((sets + 4,)),
        ],
        compiler_params=pltpu.CompilerParams(vmem_limit_bytes=limit),
        cost_estimate=pl.CostEstimate(flops=2 * 10**9, bytes_accessed=2 * MEBI, transcendentals=0),
        name="compress",
    )(*[pltpu.with_memory_space_constraint(x, pltpu.HBM) for x in (samples, rep, fwd, inv, twd)])


def doppler_kernel(x_ref, tab_ref, pow_ref, low_edge_ref, high_edge_ref, mid_ref, part_ref):
    channels = pow_ref.shape[0]
    sets = x_ref.shape[1] // (2 * ROWS)
    halves = sets // channels
    for i in range(sets):
        c, half = i // halves, i % halves

        def load(s, i=i):
            return tuple(x_ref[slot(s), i * 2 * ROWS + part * ROWS : i * 2 * ROWS + (part + 1) * ROWS, :] for part in range(2))

        def keep(j, value, i=i):
            mid_ref[i, 0, j], mid_ref[i, 1, j] = value

        def fetch(j, i=i):
            return (mid_ref[i, 0, j], mid_ref[i, 1, j])

        def store(k, value, c=c, half=half):
            tile, d1 = k // ROWS, k % ROWS
            for part in range(2):
                at = (d1 * 2 + part) * FINE + half * ROWS
                part_ref[tile, at : at + ROWS, c * LANES : (c + 1) * LANES] = value[part]

        fft32(load, keep, fetch, store, -1)
    scale = INPUT_SCALE * INPUT_SCALE / (float(RANGE) * float(RANGE) * PULSES)
    for tile in range(FAN // ROWS):
        high, low = split(part_ref[tile])
        out = dot(tab_ref[tile, 0], high) + dot(tab_ref[tile, 0], low) + dot(tab_ref[tile, 1], high)
        half = out.shape[0] // 2
        power = (out[:half] * out[:half] + out[half:] * out[half:]) * scale
        for d2 in range(FINE):
            for c in range(channels):
                at = d2 * FAN + tile * ROWS
                pow_ref[c, at : at + ROWS, :] = power[d2 * ROWS : (d2 + 1) * ROWS, c * LANES : (c + 1) * LANES]
    rows = PULSES // PACK
    lane = lax.broadcasted_iota(jnp.int32, (rows, LANES), 1)
    for c in range(channels):
        low_piece = high_piece = None
        for b in range(PACK):
            x = pow_ref[c, b * rows : (b + 1) * rows, :]
            low = pltpu.roll(x, b * PARTS, 1) if b else x
            shift = (b * PARTS - (LANES - PARTS)) % LANES
            high = pltpu.roll(x, shift, 1) if shift else x
            mine = lane >= b * PARTS
            low_piece = low if low_piece is None else jnp.where(mine, low, low_piece)
            high_piece = high if high_piece is None else jnp.where(mine, high, high_piece)
        low_edge_ref[c * rows : (c + 1) * rows, :] = low_piece
        high_edge_ref[c * rows : (c + 1) * rows, :] = high_piece


def doppler(received, channels, limit):
    sets = received.shape[1] // (2 * ROWS)
    vmem = pl.BlockSpec(memory_space=pltpu.VMEM)
    edge = pltpu.VMEM((channels * PULSES // PACK, LANES), F32)
    tables = jnp.asarray(doppler_tables())
    return pl.pallas_call(
        doppler_kernel,
        out_shape=(pltpu.VMEM((channels, PULSES, LANES), F32), edge, edge),
        in_specs=[vmem, vmem],
        out_specs=(vmem, vmem, vmem),
        scratch_shapes=[
            pltpu.VMEM((sets, 2, FAN, ROWS, LANES), F32),
            pltpu.VMEM((FAN // ROWS, 2 * FINE * ROWS, channels * LANES), F32),
        ],
        compiler_params=pltpu.CompilerParams(vmem_limit_bytes=limit),
        cost_estimate=pl.CostEstimate(flops=2 * 10**9, bytes_accessed=2 * MEBI, transcendentals=0),
        name="doppler",
    )(
        pltpu.with_memory_space_constraint(received, pltpu.VMEM),
        pltpu.with_memory_space_constraint(tables, pltpu.VMEM),
    )


def windows_kernel(groups, window_ref, thresh_ref, place_ref, core_ref, side_ref, line_ref):
    channels = window_ref.shape[0]
    total = groups * LANES
    gate = lax.broadcasted_iota(jnp.int32, (ROWS, LANES), 1) + place_ref[0] * LANES
    row_id = lax.broadcasted_iota(jnp.int32, (LANES, LANES), 0)
    col_id = lax.broadcasted_iota(jnp.int32, (LANES, LANES), 1)
    piece, inner = row_id // PARTS, row_id % PARTS
    core_ref[...] = jnp.zeros_like(core_ref)
    for c in range(channels):
        guard, train = window_ref[c, 0], window_ref[c, 1]
        reach = guard + train

        def band(offset, extra=True):
            distance = jnp.abs(offset)
            return jnp.where((distance > guard) & (distance <= reach) & extra, 1.0, 0.0).astype(BF16)

        core_ref[c * LANES : (c + 1) * LANES, c * LANES : (c + 1) * LANES] = band(row_id - col_id)
        for b in range(PACK):
            at = b * LANES
            side_ref[c, :LANES, at : at + LANES] = band(inner - PARTS - col_id, piece == b)
            side_ref[c, LANES:, at : at + LANES] = band(inner + LANES - col_id, piece == b)
        ahead = total - 1 - gate
        cells = jnp.minimum(gate, reach) - jnp.minimum(gate, guard)
        cells = cells + jnp.minimum(ahead, reach) - jnp.minimum(ahead, guard)
        line_ref[c, 0] = cells.astype(F32)
        over = jnp.zeros((ROWS, LANES), F32) + thresh_ref[c, 1].astype(F32)
        line_ref[c, 1] = over / thresh_ref[c, 0].astype(F32)


def windows(window, thresh, place, groups, limit):
    channels = window.shape[0]
    vmem = pl.BlockSpec(memory_space=pltpu.VMEM)
    smem = pl.BlockSpec(memory_space=pltpu.SMEM)
    return pl.pallas_call(
        functools.partial(windows_kernel, groups),
        out_shape=(
            pltpu.VMEM((channels * LANES, channels * LANES), BF16),
            pltpu.VMEM((channels, 2 * LANES, PACK * LANES), BF16),
            pltpu.VMEM((channels, 2, ROWS, LANES), F32),
        ),
        in_specs=[smem, smem, smem],
        out_specs=(vmem, vmem, vmem),
        compiler_params=pltpu.CompilerParams(vmem_limit_bytes=limit),
        cost_estimate=pl.CostEstimate(flops=10**7, bytes_accessed=MEBI, transcendentals=0),
        name="windows",
    )(window, thresh, place)


def core_kernel(pow_ref, band_ref, noise_ref):
    channels = pow_ref.shape[0]
    high, low = split(jnp.concatenate([pow_ref[c] for c in range(channels)], axis=1))
    noise = dot(high, band_ref[...]) + dot(low, band_ref[...])
    for c in range(channels):
        noise_ref[c] = noise[:, c * LANES : (c + 1) * LANES]


def core(power, band, limit):
    vmem = pl.BlockSpec(memory_space=pltpu.VMEM)
    return pl.pallas_call(
        core_kernel,
        out_shape=pltpu.VMEM(power.shape, F32),
        in_specs=[vmem, vmem],
        out_specs=vmem,
        compiler_params=pltpu.CompilerParams(vmem_limit_bytes=limit),
        cost_estimate=pl.CostEstimate(flops=2 * 10**9, bytes_accessed=MEBI, transcendentals=0),
        name="core",
    )(in_vmem(power), in_vmem(band))


def in_vmem(x):
    return pltpu.with_memory_space_constraint(x, pltpu.VMEM)


def cfar_kernel(pow_ref, noise_ref, left_ref, right_ref, side_ref, line_ref, ratio_ref, soft_ref):
    channels = pow_ref.shape[0]
    rows = PULSES // PACK
    soft_sum = jnp.zeros((ROWS, LANES), F32)
    for c in range(channels):
        halo = jnp.concatenate([ref[c * rows : (c + 1) * rows, :] for ref in (left_ref, right_ref)], axis=1)
        high, low = split(halo)
        side = dot(high, side_ref[c]) + dot(low, side_ref[c])
        cells = jnp.concatenate([line_ref[c, 0]] * (rows // ROWS), axis=0)
        over = jnp.concatenate([line_ref[c, 1]] * (rows // ROWS), axis=0)
        for b in range(PACK):
            at = b * rows
            noise = noise_ref[c, at : at + rows, :] + side[:, b * LANES : (b + 1) * LANES]
            ratio = pow_ref[c, at : at + rows, :] * cells / (noise + EPSILON)
            ratio_ref[c, at : at + rows, :] = ratio
            soft = jnp.clip(ratio * over - 1.0, 0.0, 1.0)
            soft_sum = soft_sum + soft.reshape(rows // ROWS, ROWS, LANES).sum(axis=0)
    soft_ref[...] = jnp.broadcast_to(jnp.sum(soft_sum, axis=0, keepdims=True), soft_ref.shape)


def cfar(power, noise, left, right, side, line, peers, limit):
    vmem = pl.BlockSpec(memory_space=pltpu.VMEM)
    return pl.pallas_call(
        cfar_kernel,
        out_shape=(pltpu.VMEM(power.shape, F32), pltpu.VMEM((peers, LANES), F32)),
        in_specs=[vmem] * 6,
        out_specs=(vmem, vmem),
        compiler_params=pltpu.CompilerParams(vmem_limit_bytes=limit),
        cost_estimate=pl.CostEstimate(flops=10**9, bytes_accessed=2 * MEBI, transcendentals=0),
        name="cfar",
    )(*[in_vmem(x) for x in (power, noise, left, right, side, line)])


def local(samples, replica, window, thresh):
    groups = lax.axis_size("pulse")
    channels = samples.shape[1]
    assert samples.shape[3] == RANGE and groups == FAN and samples.shape[2] == FINE
    limit = 24 * MEBI
    ready = compress(samples, replica, limit)
    received = lax.all_to_all(ready, "pulse", 0, 0, axis_index_groups=[ORDER])
    place = lax.axis_index("pulse").reshape(1)
    band, side, line = windows(window, thresh, place, groups, limit)
    power, low_edge, high_edge = doppler(received, channels, limit)
    ends = groups - 1
    left = lax.ppermute(high_edge, "pulse", [(i, i + 1) for i in range(ends)])
    right = lax.ppermute(low_edge, "pulse", [(i + 1, i) for i in range(ends)])
    noise = core(power, band, limit)
    peers = lax.axis_size("chan") * lax.axis_size("sub")
    ratio_map, soft = cfar(power, noise, left, right, side, line, peers, limit)
    plane = jnp.sum(lax.all_to_all(soft.reshape(peers, 1, LANES), ("chan", "sub"), 0, 0), axis=0, keepdims=True)
    counts = lax.all_to_all(jnp.broadcast_to(plane, (groups, 1, LANES)), "pulse", 0, 0)
    detections = jnp.sum(counts) * (1024.0 / (PULSES * RANGE))
    return (ratio_map, detections.reshape(1))


def solution(mesh):
    in_specs = (
        P(None, ("grp", "chan", "sub"), "pulse", None),
        P(),
        P(("grp", "chan", "sub"), None),
        P(("grp", "chan", "sub"), None),
    )
    out_specs = (P(("grp", "chan", "sub"), None, "pulse"), P("grp"))
    return jax.shard_map(local, mesh=mesh, in_specs=in_specs, out_specs=out_specs, check_vma=False)
```

```python
import functools
import math

import jax
import jax.numpy as jnp
import numpy as np
from jax import lax
from jax.experimental import pallas as pl
from jax.experimental.pallas import tpu as pltpu
from jax.sharding import PartitionSpec as P

PULSES = 512
RANGE = 4096
GUARD_MAX = 4
TRAIN_MAX = 28

EPSILON = 1e-06
INPUT_SCALE = 1.0 / 2048.0
MARGIN = GUARD_MAX + TRAIN_MAX

LANES = 128
ROWS = 8
FAN = 32
TAIL = RANGE // FAN
FINE = PULSES // FAN
PARTS = MARGIN
PACK = LANES // PARTS
F32 = jnp.float32
BF16 = jnp.bfloat16
MEBI = 1 << 20
ORDER = [place ^ (place >> 1) for place in range(FAN)]


def slot(device):
    return ORDER.index(device)


def split_table(table):
    high = table.astype(BF16)
    low = (table - high.astype(np.float64)).astype(BF16)
    return np.stack([high, low])


def unit(product, period):
    angle = 2.0 * np.pi / period * (np.asarray(product, np.int64) % period)
    return np.cos(angle), np.sin(angle)


def range_tables():
    b = np.arange(TAIL)[:, None]
    col = np.arange(TAIL)[None, :]
    freq = 4 * (col % FAN) + col // FAN
    cos, sin = unit(b * freq, TAIL)
    forward = np.block([[cos, -sin], [sin, cos]])
    inverse = forward.T
    k1 = np.arange(FAN)[:, None]
    cos, sin = unit(k1 * np.arange(TAIL)[None, :], RANGE)
    twiddle = np.stack([cos, sin]).astype(np.float32)
    return split_table(forward), split_table(inverse), twiddle


def doppler_tables():
    tiles = []
    for t in range(FAN // ROWS):
        table = np.zeros((2, FINE, ROWS, ROWS, 2, FINE))
        for d1 in range(ROWS):
            bins = 8 * t + d1 + FAN * np.arange(FINE)[:, None]
            cos, sin = unit(bins * np.arange(FINE)[None, :], PULSES)
            table[0, :, d1, d1, 0] = cos
            table[0, :, d1, d1, 1] = sin
            table[1, :, d1, d1, 0] = -sin
            table[1, :, d1, d1, 1] = cos
        tiles.append(split_table(table.reshape(2 * PULSES // 4, 2 * PULSES // 4)))
    return np.stack(tiles)


def add(x, y):
    return (x[0] + y[0], x[1] + y[1])


def sub(x, y):
    return (x[0] - y[0], x[1] - y[1])


def turn(x, sign):
    return (-x[1], x[0]) if sign > 0 else (x[1], -x[0])


def add_turn(x, y, sign):
    if sign > 0:
        return (x[0] - y[1], x[1] + y[0])
    return (x[0] + y[1], x[1] - y[0])


def by_constant(x, index, period, sign):
    index = index % period
    if index == 0:
        return x
    angle = 2.0 * math.pi * index / period
    cos, sin = math.cos(angle), sign * math.sin(angle)
    if 8 * index == period:
        return ((x[0] - x[1]) * cos, (x[0] + x[1]) * cos) if sign > 0 else ((x[0] + x[1]) * cos, (x[1] - x[0]) * cos)
    if 4 * index == period:
        return turn(x, sign)
    return (x[0] * cos - x[1] * sin, x[0] * sin + x[1] * cos)


def fft4(x, sign):
    a, b = add(x[0], x[2]), sub(x[0], x[2])
    c, d = add(x[1], x[3]), sub(x[1], x[3])
    return [add(a, c), add_turn(b, d, sign), sub(a, c), add_turn(b, d, -sign)]


def fft8(x, sign):
    even, odd = fft4(x[0::2], sign), fft4(x[1::2], sign)
    root = math.sqrt(0.5)
    out = [None] * 8
    out[0], out[4] = add(even[0], odd[0]), sub(even[0], odd[0])
    out[2], out[6] = add_turn(even[2], odd[2], sign), add_turn(even[2], odd[2], -sign)
    for k in (1, 3):
        o = odd[k]
        if k == 1:
            w = (o[0] - o[1], o[0] + o[1]) if sign > 0 else (o[0] + o[1], o[1] - o[0])
        else:
            w = (-o[0] - o[1], o[0] - o[1]) if sign > 0 else (o[1] - o[0], -o[0] - o[1])
        w = (w[0] * root, w[1] * root)
        out[k], out[k + 4] = add(even[k], w), sub(even[k], w)
    return out


def fft32(load, keep, fetch, store, sign):
    for n2 in range(8):
        mid = fft4([load(n2 + 8 * n1) for n1 in range(4)], sign)
        for k1 in range(4):
            keep(k1 * 8 + n2, by_constant(mid[k1], n2 * k1, 32, sign))
    for k1 in range(4):
        out = fft8([fetch(k1 * 8 + n2) for n2 in range(8)], sign)
        for k2 in range(8):
            store(k1 + 4 * k2, out[k2])


def split(x):
    high = x.astype(BF16)
    return high, (x - high.astype(F32)).astype(BF16)


def dot(x, y):
    return jnp.dot(x, y, preferred_element_type=F32)


def compress_kernel(
    x_hbm, rep_hbm, fwd_hbm, inv_hbm, twd_hbm, o_ref,
    x_ref, rep_ref, fwd_ref, inv_ref, twd_ref, h_ref, mid_ref, high_ref, low_ref, out_ref, sems,
):
    channels, pulses = x_hbm.shape[1], x_hbm.shape[2]
    sets = [(c, p) for c in range(channels) for p in range(0, pulses, ROWS)]
    loads = [
        pltpu.make_async_copy(x_hbm.at[:, c, pl.ds(p, ROWS)], x_ref.at[i], sems.at[i]) for i, (c, p) in enumerate(sets)
    ]
    n = len(sets)
    load_rep = pltpu.make_async_copy(rep_hbm, rep_ref, sems.at[n])
    load_twd = pltpu.make_async_copy(twd_hbm, twd_ref, sems.at[n + 1])
    load_fwd = pltpu.make_async_copy(fwd_hbm, fwd_ref, sems.at[n + 2])
    load_inv = pltpu.make_async_copy(inv_hbm, inv_ref, sems.at[n + 3])
    for load in [loads[0], load_rep, load_twd, load_fwd, *loads[1:], load_inv]:
        load.start()

    load_rep.wait()
    for part in range(2):
        turned = rep_ref[pl.ds(part, FAN, stride=2), :].T
        h_ref[part] = jnp.concatenate([turned[q * FAN : (q + 1) * FAN] for q in range(4)], axis=1)
    load_twd.wait()

    def row(ref, part, k):
        return jnp.broadcast_to(ref[part, k : k + 1, :], (ROWS, LANES))

    def put(i, k, value):
        at = (i * FAN + k) * ROWS
        for part in range(2):
            high, low = split(value[part])
            high_ref[at : at + ROWS, part * LANES : (part + 1) * LANES] = high
            low_ref[at : at + ROWS, part * LANES : (part + 1) * LANES] = low

    def product(table):
        for t in range(4):
            at = pl.ds(t * 256, 256)
            high = high_ref[at]
            out_ref[at] = dot(high, table[0]) + dot(low_ref[at], table[0]) + dot(high, table[1])

    for i in range(n):
        loads[i].wait()

        def load(a, i=i):
            return tuple(x_ref[i, part, :, a * LANES : (a + 1) * LANES].astype(F32) for part in range(2))

        def keep(j, value, i=i):
            mid_ref[i, 0, j], mid_ref[i, 1, j] = value

        def fetch(j, i=i):
            return (mid_ref[i, 0, j], mid_ref[i, 1, j])

        def twisted(k, value, i=i):
            cos, sin = row(twd_ref, 0, k), row(twd_ref, 1, k)
            put(i, k, (value[0] * cos + value[1] * sin, value[1] * cos - value[0] * sin))

        fft32(load, keep, fetch, twisted, -1)
    load_fwd.wait()
    product(fwd_ref)
    for i in range(n):
        for k in range(FAN):
            at = (i * FAN + k) * ROWS
            re, im = out_ref[at : at + ROWS, :LANES], out_ref[at : at + ROWS, LANES:]
            h_re, h_im = row(h_ref, 0, k), row(h_ref, 1, k)
            put(i, k, (re * h_re - im * h_im, re * h_im + im * h_re))
    load_inv.wait()
    product(inv_ref)
    for i in range(n):

        def keep(j, value, i=i):
            mid_ref[i, 0, j], mid_ref[i, 1, j] = value

        def fetch(j, i=i):
            return (mid_ref[i, 0, j], mid_ref[i, 1, j])

        def untwisted(k, i=i):
            at = (i * FAN + k) * ROWS
            re, im = out_ref[at : at + ROWS, :LANES], out_ref[at : at + ROWS, LANES:]
            cos, sin = row(twd_ref, 0, k), row(twd_ref, 1, k)
            return (re * cos - im * sin, im * cos + re * sin)

        def store(a, value, i=i):
            for part in range(2):
                o_ref[slot(a), i * 2 * ROWS + part * ROWS : i * 2 * ROWS + (part + 1) * ROWS, :] = value[part]

        fft32(untwisted, keep, fetch, store, 1)


def compress(samples, replica, limit):
    fwd, inv, twd = [jnp.asarray(table) for table in range_tables()]
    sets = samples.shape[1] * samples.shape[2] // ROWS
    rep = replica.reshape(2, FAN, LANES).transpose(1, 0, 2).reshape(2 * FAN, LANES)
    any_space = pl.BlockSpec(memory_space=pltpu.HBM)
    return pl.pallas_call(
        compress_kernel,
        out_shape=pltpu.VMEM((FAN, sets * 2 * ROWS, LANES), F32),
        in_specs=[any_space] * 5,
        out_specs=pl.BlockSpec(memory_space=pltpu.VMEM),
        scratch_shapes=[
            pltpu.VMEM((sets, 2, ROWS, RANGE), jnp.int32),
            pltpu.VMEM((2 * FAN, LANES), F32),
            pltpu.VMEM((2, 2 * TAIL, 2 * TAIL), BF16),
            pltpu.VMEM((2, 2 * TAIL, 2 * TAIL), BF16),
            pltpu.VMEM((2, FAN, LANES), F32),
            pltpu.VMEM((2, FAN, LANES), F32),
            pltpu.VMEM((sets, 2, FAN, ROWS, LANES), F32),
            pltpu.VMEM((sets * FAN * ROWS, 2 * LANES), BF16),
            pltpu.VMEM((sets * FAN * ROWS, 2 * LANES), BF16),
            pltpu.VMEM((sets * FAN * ROWS, 2 * LANES), F32),
            pltpu.SemaphoreType.DMA((sets + 4,)),
        ],
        compiler_params=pltpu.CompilerParams(vmem_limit_bytes=limit),
        cost_estimate=pl.CostEstimate(flops=2 * 10**9, bytes_accessed=2 * MEBI, transcendentals=0),
        name="compress",
    )(*[pltpu.with_memory_space_constraint(x, pltpu.HBM) for x in (samples, rep, fwd, inv, twd)])


def doppler_kernel(x_ref, tab_ref, pow_ref, first_ref, second_ref, mid_ref, part_ref):
    channels = pow_ref.shape[0]
    sets = x_ref.shape[1] // (2 * ROWS)
    halves = sets // channels
    for i in range(sets):
        c, half = i // halves, i % halves

        def load(s, i=i):
            return tuple(x_ref[slot(s), i * 2 * ROWS + part * ROWS : i * 2 * ROWS + (part + 1) * ROWS, :] for part in range(2))

        def keep(j, value, i=i):
            mid_ref[i, 0, j], mid_ref[i, 1, j] = value

        def fetch(j, i=i):
            return (mid_ref[i, 0, j], mid_ref[i, 1, j])

        def store(k, value, c=c, half=half):
            tile, d1 = k // ROWS, k % ROWS
            for part in range(2):
                at = (d1 * 2 + part) * FINE + half * ROWS
                part_ref[tile, at : at + ROWS, c * LANES : (c + 1) * LANES] = value[part]

        fft32(load, keep, fetch, store, -1)
    scale = INPUT_SCALE * INPUT_SCALE / (float(RANGE) * float(RANGE) * PULSES)
    for tile in range(FAN // ROWS):
        high, low = split(part_ref[tile])
        out = dot(tab_ref[tile, 0], high) + dot(tab_ref[tile, 0], low) + dot(tab_ref[tile, 1], high)
        half = out.shape[0] // 2
        power = (out[:half] * out[:half] + out[half:] * out[half:]) * scale
        for d2 in range(FINE):
            for c in range(channels):
                at = d2 * FAN + tile * ROWS
                pow_ref[c, at : at + ROWS, :] = power[d2 * ROWS : (d2 + 1) * ROWS, c * LANES : (c + 1) * LANES]
    rows = PULSES // PACK
    lane = lax.broadcasted_iota(jnp.int32, (rows, LANES), 1)
    even = lax.broadcast(lax.rem(lax.axis_index("pulse"), 2), (rows, LANES)) == 0
    for c in range(channels):
        low_piece = high_piece = None
        for b in range(PACK):
            x = pow_ref[c, b * rows : (b + 1) * rows, :]
            low = pltpu.roll(x, b * PARTS, 1) if b else x
            shift = (b * PARTS - (LANES - PARTS)) % LANES
            high = pltpu.roll(x, shift, 1) if shift else x
            mine = lane >= b * PARTS
            low_piece = low if low_piece is None else jnp.where(mine, low, low_piece)
            high_piece = high if high_piece is None else jnp.where(mine, high, high_piece)
        first_ref[c * rows : (c + 1) * rows, :] = jnp.where(even, high_piece, low_piece)
        second_ref[c * rows : (c + 1) * rows, :] = jnp.where(even, low_piece, high_piece)


def doppler(received, channels, limit):
    sets = received.shape[1] // (2 * ROWS)
    vmem = pl.BlockSpec(memory_space=pltpu.VMEM)
    edge = pltpu.VMEM((channels * PULSES // PACK, LANES), F32)
    tables = jnp.asarray(doppler_tables())
    return pl.pallas_call(
        doppler_kernel,
        out_shape=(pltpu.VMEM((channels, PULSES, LANES), F32), edge, edge),
        in_specs=[vmem, vmem],
        out_specs=(vmem, vmem, vmem),
        scratch_shapes=[
            pltpu.VMEM((sets, 2, FAN, ROWS, LANES), F32),
            pltpu.VMEM((FAN // ROWS, 2 * FINE * ROWS, channels * LANES), F32),
        ],
        compiler_params=pltpu.CompilerParams(vmem_limit_bytes=limit),
        cost_estimate=pl.CostEstimate(flops=2 * 10**9, bytes_accessed=2 * MEBI, transcendentals=0),
        name="doppler",
    )(
        pltpu.with_memory_space_constraint(received, pltpu.VMEM),
        pltpu.with_memory_space_constraint(tables, pltpu.VMEM),
    )


def windows_kernel(groups, window_ref, thresh_ref, core_ref, side_ref, line_ref):
    channels = window_ref.shape[0]
    total = groups * LANES
    gate = lax.broadcasted_iota(jnp.int32, (ROWS, LANES), 1) + lax.axis_index("pulse") * LANES
    row_id = lax.broadcasted_iota(jnp.int32, (LANES, LANES), 0)
    col_id = lax.broadcasted_iota(jnp.int32, (LANES, LANES), 1)
    piece, inner = row_id // PARTS, row_id % PARTS
    odd = lax.rem(lax.axis_index("pulse"), 2)
    first = LANES - odd * (LANES + PARTS)
    second = odd * (LANES + PARTS) - PARTS
    core_ref[...] = jnp.zeros_like(core_ref)
    for c in range(channels):
        guard, train = window_ref[c, 0], window_ref[c, 1]
        reach = guard + train

        def band(offset, extra=True):
            distance = jnp.abs(offset)
            return jnp.where((distance > guard) & (distance <= reach) & extra, 1.0, 0.0).astype(BF16)

        core_ref[c * LANES : (c + 1) * LANES, c * LANES : (c + 1) * LANES] = band(row_id - col_id)
        for b in range(PACK):
            at = b * LANES
            side_ref[c, :LANES, at : at + LANES] = band(inner + first - col_id, piece == b)
            side_ref[c, LANES:, at : at + LANES] = band(inner + second - col_id, piece == b)
        ahead = total - 1 - gate
        cells = jnp.minimum(gate, reach) - jnp.minimum(gate, guard)
        cells = cells + jnp.minimum(ahead, reach) - jnp.minimum(ahead, guard)
        line_ref[c, 0] = cells.astype(F32)
        over = jnp.zeros((ROWS, LANES), F32) + thresh_ref[c, 1].astype(F32)
        line_ref[c, 1] = over / thresh_ref[c, 0].astype(F32)


def windows(window, thresh, groups, limit):
    channels = window.shape[0]
    vmem = pl.BlockSpec(memory_space=pltpu.VMEM)
    smem = pl.BlockSpec(memory_space=pltpu.SMEM)
    return pl.pallas_call(
        functools.partial(windows_kernel, groups),
        out_shape=(
            pltpu.VMEM((channels * LANES, channels * LANES), BF16),
            pltpu.VMEM((channels, 2 * LANES, PACK * LANES), BF16),
            pltpu.VMEM((channels, 2, ROWS, LANES), F32),
        ),
        in_specs=[smem, smem],
        out_specs=(vmem, vmem, vmem),
        compiler_params=pltpu.CompilerParams(vmem_limit_bytes=limit),
        cost_estimate=pl.CostEstimate(flops=10**7, bytes_accessed=MEBI, transcendentals=0),
        name="windows",
    )(window, thresh)


def core_kernel(pow_ref, band_ref, noise_ref):
    channels = pow_ref.shape[0]
    high, low = split(jnp.concatenate([pow_ref[c] for c in range(channels)], axis=1))
    noise = dot(high, band_ref[...]) + dot(low, band_ref[...])
    for c in range(channels):
        noise_ref[c] = noise[:, c * LANES : (c + 1) * LANES]


def core(power, band, limit):
    vmem = pl.BlockSpec(memory_space=pltpu.VMEM)
    return pl.pallas_call(
        core_kernel,
        out_shape=pltpu.VMEM(power.shape, F32),
        in_specs=[vmem, vmem],
        out_specs=vmem,
        compiler_params=pltpu.CompilerParams(vmem_limit_bytes=limit),
        cost_estimate=pl.CostEstimate(flops=2 * 10**9, bytes_accessed=MEBI, transcendentals=0),
        name="core",
    )(in_vmem(power), in_vmem(band))


def in_vmem(x):
    return pltpu.with_memory_space_constraint(x, pltpu.VMEM)


def cfar_kernel(pow_ref, noise_ref, first_ref, second_ref, side_ref, line_ref, out_hbm, soft_ref, ratio_ref, sems):
    channels = pow_ref.shape[0]
    stores = []
    rows = PULSES // PACK
    soft_sum = jnp.zeros((ROWS, LANES), F32)
    for c in range(channels):
        halo = jnp.concatenate([ref[c * rows : (c + 1) * rows, :] for ref in (first_ref, second_ref)], axis=1)
        high, low = split(halo)
        side = dot(high, side_ref[c]) + dot(low, side_ref[c])
        cells = jnp.concatenate([line_ref[c, 0]] * (rows // ROWS), axis=0)
        over = jnp.concatenate([line_ref[c, 1]] * (rows // ROWS), axis=0)
        for b in range(PACK):
            at = b * rows
            noise = noise_ref[c, at : at + rows, :] + side[:, b * LANES : (b + 1) * LANES]
            ratio = pow_ref[c, at : at + rows, :] * cells / (noise + EPSILON)
            ratio_ref[c, at : at + rows, :] = ratio
            piece = (c, pl.ds(at, rows))
            stores.append(pltpu.make_async_copy(ratio_ref.at[piece], out_hbm.at[piece], sems.at[len(stores)]))
            stores[-1].start()
            soft = jnp.clip(ratio * over - 1.0, 0.0, 1.0)
            soft_sum = soft_sum + soft.reshape(rows // ROWS, ROWS, LANES).sum(axis=0)
    soft_ref[...] = jnp.broadcast_to(jnp.sum(soft_sum, axis=0, keepdims=True), soft_ref.shape)
    for store in stores:
        store.wait()


def cfar(power, noise, first, second, side, line, peers, limit):
    vmem = pl.BlockSpec(memory_space=pltpu.VMEM)
    return pl.pallas_call(
        cfar_kernel,
        out_shape=(pltpu.HBM(power.shape, F32), pltpu.VMEM((peers, LANES), F32)),
        in_specs=[vmem] * 6,
        out_specs=(pl.BlockSpec(memory_space=pltpu.HBM), vmem),
        scratch_shapes=[
            pltpu.VMEM(power.shape, F32),
            pltpu.SemaphoreType.DMA((power.shape[0] * PACK,)),
        ],
        compiler_params=pltpu.CompilerParams(vmem_limit_bytes=limit),
        cost_estimate=pl.CostEstimate(flops=10**9, bytes_accessed=2 * MEBI, transcendentals=0),
        name="cfar",
    )(*[in_vmem(x) for x in (power, noise, first, second, side, line)])


def local(samples, replica, window, thresh):
    groups = lax.axis_size("pulse")
    channels = samples.shape[1]
    assert samples.shape[3] == RANGE and groups == FAN and samples.shape[2] == FINE
    limit = 24 * MEBI
    ready = compress(samples, replica, limit)
    received = lax.all_to_all(ready, "pulse", 0, 0, axis_index_groups=[ORDER])
    power, first, second = doppler(received, channels, limit)
    window, first = lax.optimization_barrier((window, first))
    band, side, line = windows(window, thresh, groups, limit)
    first = lax.ppermute(first, "pulse", [(i, i ^ 1) for i in range(groups)])
    second = lax.ppermute(second, "pulse", [(i, ((i + 1) ^ 1) - 1) for i in range(1, groups - 1)])
    noise = core(power, band, limit)
    peers = lax.axis_size("chan") * lax.axis_size("sub")
    ratio_map, soft = cfar(power, noise, first, second, side, line, peers, limit)
    plane = jnp.sum(lax.all_to_all(soft.reshape(peers, 1, LANES), ("chan", "sub"), 0, 0), axis=0, keepdims=True)
    counts = lax.all_to_all(jnp.broadcast_to(plane, (groups, 1, LANES)), "pulse", 0, 0)
    detections = jnp.sum(counts) * (1024.0 / (PULSES * RANGE))
    return (ratio_map, detections.reshape(1))


def solution(mesh):
    in_specs = (
        P(None, ("grp", "chan", "sub"), "pulse", None),
        P(),
        P(("grp", "chan", "sub"), None),
        P(("grp", "chan", "sub"), None),
    )
    out_specs = (P(("grp", "chan", "sub"), None, "pulse"), P("grp"))
    return jax.shard_map(local, mesh=mesh, in_specs=in_specs, out_specs=out_specs, check_vma=False)
```

```python
import functools
import math

import jax
import jax.numpy as jnp
import numpy as np
from jax import lax
from jax.experimental import pallas as pl
from jax.experimental.pallas import tpu as pltpu
from jax.sharding import PartitionSpec as P

PULSES = 512
RANGE = 4096
GUARD_MAX = 4
TRAIN_MAX = 28

EPSILON = 1e-06
INPUT_SCALE = 1.0 / 2048.0
MARGIN = GUARD_MAX + TRAIN_MAX

LANES = 128
ROWS = 8
FAN = 32
TAIL = RANGE // FAN
FINE = PULSES // FAN
PARTS = MARGIN
PACK = LANES // PARTS
F32 = jnp.float32
BF16 = jnp.bfloat16
MEBI = 1 << 20
ORDER = [place ^ (place >> 1) for place in range(FAN)]


def slot(device):
    return ORDER.index(device)


def split_table(table):
    high = table.astype(BF16)
    low = (table - high.astype(np.float64)).astype(BF16)
    return np.stack([high, low])


def unit(product, period):
    angle = 2.0 * np.pi / period * (np.asarray(product, np.int64) % period)
    return np.cos(angle), np.sin(angle)


def range_tables():
    b = np.arange(TAIL)[:, None]
    col = np.arange(TAIL)[None, :]
    freq = 4 * (col % FAN) + col // FAN
    cos, sin = unit(b * freq, TAIL)
    forward = np.block([[cos, -sin], [sin, cos]])
    inverse = forward.T
    k1 = np.arange(FAN)[:, None]
    cos, sin = unit(k1 * np.arange(TAIL)[None, :], RANGE)
    twiddle = np.stack([cos, sin]).astype(np.float32)
    return split_table(forward), split_table(inverse), twiddle


def doppler_tables():
    tiles = []
    for t in range(FAN // ROWS):
        table = np.zeros((2, FINE, ROWS, ROWS, 2, FINE))
        for d1 in range(ROWS):
            bins = 8 * t + d1 + FAN * np.arange(FINE)[:, None]
            cos, sin = unit(bins * np.arange(FINE)[None, :], PULSES)
            table[0, :, d1, d1, 0] = cos
            table[0, :, d1, d1, 1] = sin
            table[1, :, d1, d1, 0] = -sin
            table[1, :, d1, d1, 1] = cos
        tiles.append(split_table(table.reshape(2 * PULSES // 4, 2 * PULSES // 4)))
    return np.stack(tiles)


def add(x, y):
    return (x[0] + y[0], x[1] + y[1])


def sub(x, y):
    return (x[0] - y[0], x[1] - y[1])


def turn(x, sign):
    return (-x[1], x[0]) if sign > 0 else (x[1], -x[0])


def add_turn(x, y, sign):
    if sign > 0:
        return (x[0] - y[1], x[1] + y[0])
    return (x[0] + y[1], x[1] - y[0])


def by_constant(x, index, period, sign):
    index = index % period
    if index == 0:
        return x
    angle = 2.0 * math.pi * index / period
    cos, sin = math.cos(angle), sign * math.sin(angle)
    if 8 * index == period:
        return ((x[0] - x[1]) * cos, (x[0] + x[1]) * cos) if sign > 0 else ((x[0] + x[1]) * cos, (x[1] - x[0]) * cos)
    if 4 * index == period:
        return turn(x, sign)
    return (x[0] * cos - x[1] * sin, x[0] * sin + x[1] * cos)


def fft4(x, sign):
    a, b = add(x[0], x[2]), sub(x[0], x[2])
    c, d = add(x[1], x[3]), sub(x[1], x[3])
    return [add(a, c), add_turn(b, d, sign), sub(a, c), add_turn(b, d, -sign)]


def fft8(x, sign):
    even, odd = fft4(x[0::2], sign), fft4(x[1::2], sign)
    root = math.sqrt(0.5)
    out = [None] * 8
    out[0], out[4] = add(even[0], odd[0]), sub(even[0], odd[0])
    out[2], out[6] = add_turn(even[2], odd[2], sign), add_turn(even[2], odd[2], -sign)
    for k in (1, 3):
        o = odd[k]
        if k == 1:
            w = (o[0] - o[1], o[0] + o[1]) if sign > 0 else (o[0] + o[1], o[1] - o[0])
        else:
            w = (-o[0] - o[1], o[0] - o[1]) if sign > 0 else (o[1] - o[0], -o[0] - o[1])
        w = (w[0] * root, w[1] * root)
        out[k], out[k + 4] = add(even[k], w), sub(even[k], w)
    return out


def fft32(load, keep, fetch, store, sign):
    for n2 in range(8):
        mid = fft4([load(n2 + 8 * n1) for n1 in range(4)], sign)
        for k1 in range(4):
            keep(k1 * 8 + n2, by_constant(mid[k1], n2 * k1, 32, sign))
    for k1 in range(4):
        out = fft8([fetch(k1 * 8 + n2) for n2 in range(8)], sign)
        for k2 in range(8):
            store(k1 + 4 * k2, out[k2])


def split(x):
    high = x.astype(BF16)
    return high, (x - high.astype(F32)).astype(BF16)


def dot(x, y):
    return jnp.dot(x, y, preferred_element_type=F32)


def compress_kernel(
    x_hbm, rep_hbm, fwd_hbm, inv_hbm, twd_hbm, o_ref,
    x_ref, rep_ref, fwd_ref, inv_ref, twd_ref, h_ref, mid_ref, high_ref, low_ref, out_ref, sems,
):
    channels, pulses = x_hbm.shape[1], x_hbm.shape[2]
    sets = [(c, p) for c in range(channels) for p in range(0, pulses, ROWS)]
    loads = [
        pltpu.make_async_copy(x_hbm.at[:, c, pl.ds(p, ROWS)], x_ref.at[i], sems.at[i]) for i, (c, p) in enumerate(sets)
    ]
    n = len(sets)
    load_rep = pltpu.make_async_copy(rep_hbm, rep_ref, sems.at[n])
    load_twd = pltpu.make_async_copy(twd_hbm, twd_ref, sems.at[n + 1])
    load_fwd = pltpu.make_async_copy(fwd_hbm, fwd_ref, sems.at[n + 2])
    load_inv = pltpu.make_async_copy(inv_hbm, inv_ref, sems.at[n + 3])
    for load in [loads[0], load_rep, load_twd, load_fwd, *loads[1:], load_inv]:
        load.start()

    load_rep.wait()
    for part in range(2):
        turned = rep_ref[pl.ds(part, FAN, stride=2), :].T
        h_ref[part] = jnp.concatenate([turned[q * FAN : (q + 1) * FAN] for q in range(4)], axis=1)
    load_twd.wait()

    def row(ref, part, k):
        return jnp.broadcast_to(ref[part, k : k + 1, :], (ROWS, LANES))

    def put(i, k, value):
        at = (i * FAN + k) * ROWS
        for part in range(2):
            high, low = split(value[part])
            high_ref[at : at + ROWS, part * LANES : (part + 1) * LANES] = high
            low_ref[at : at + ROWS, part * LANES : (part + 1) * LANES] = low

    def product(table):
        for t in range(4):
            at = pl.ds(t * 256, 256)
            high = high_ref[at]
            out_ref[at] = dot(high, table[0]) + dot(low_ref[at], table[0]) + dot(high, table[1])

    for i in range(n):
        loads[i].wait()

        def load(a, i=i):
            return tuple(x_ref[i, part, :, a * LANES : (a + 1) * LANES].astype(F32) for part in range(2))

        def keep(j, value, i=i):
            mid_ref[i, 0, j], mid_ref[i, 1, j] = value

        def fetch(j, i=i):
            return (mid_ref[i, 0, j], mid_ref[i, 1, j])

        def twisted(k, value, i=i):
            cos, sin = row(twd_ref, 0, k), row(twd_ref, 1, k)
            put(i, k, (value[0] * cos + value[1] * sin, value[1] * cos - value[0] * sin))

        fft32(load, keep, fetch, twisted, -1)
    load_fwd.wait()
    product(fwd_ref)
    for i in range(n):
        for k in range(FAN):
            at = (i * FAN + k) * ROWS
            re, im = out_ref[at : at + ROWS, :LANES], out_ref[at : at + ROWS, LANES:]
            h_re, h_im = row(h_ref, 0, k), row(h_ref, 1, k)
            put(i, k, (re * h_re - im * h_im, re * h_im + im * h_re))
    load_inv.wait()
    product(inv_ref)
    for i in range(n):

        def keep(j, value, i=i):
            mid_ref[i, 0, j], mid_ref[i, 1, j] = value

        def fetch(j, i=i):
            return (mid_ref[i, 0, j], mid_ref[i, 1, j])

        def untwisted(k, i=i):
            at = (i * FAN + k) * ROWS
            re, im = out_ref[at : at + ROWS, :LANES], out_ref[at : at + ROWS, LANES:]
            cos, sin = row(twd_ref, 0, k), row(twd_ref, 1, k)
            return (re * cos - im * sin, im * cos + re * sin)

        def store(a, value, i=i):
            for part in range(2):
                o_ref[slot(a), i * 2 * ROWS + part * ROWS : i * 2 * ROWS + (part + 1) * ROWS, :] = value[part]

        fft32(untwisted, keep, fetch, store, 1)


def compress(samples, replica, limit):
    fwd, inv, twd = [jnp.asarray(table) for table in range_tables()]
    sets = samples.shape[1] * samples.shape[2] // ROWS
    rep = replica.reshape(2, FAN, LANES).transpose(1, 0, 2).reshape(2 * FAN, LANES)
    any_space = pl.BlockSpec(memory_space=pltpu.HBM)
    return pl.pallas_call(
        compress_kernel,
        out_shape=pltpu.VMEM((FAN, sets * 2 * ROWS, LANES), F32),
        in_specs=[any_space] * 5,
        out_specs=pl.BlockSpec(memory_space=pltpu.VMEM),
        scratch_shapes=[
            pltpu.VMEM((sets, 2, ROWS, RANGE), jnp.int32),
            pltpu.VMEM((2 * FAN, LANES), F32),
            pltpu.VMEM((2, 2 * TAIL, 2 * TAIL), BF16),
            pltpu.VMEM((2, 2 * TAIL, 2 * TAIL), BF16),
            pltpu.VMEM((2, FAN, LANES), F32),
            pltpu.VMEM((2, FAN, LANES), F32),
            pltpu.VMEM((sets, 2, FAN, ROWS, LANES), F32),
            pltpu.VMEM((sets * FAN * ROWS, 2 * LANES), BF16),
            pltpu.VMEM((sets * FAN * ROWS, 2 * LANES), BF16),
            pltpu.VMEM((sets * FAN * ROWS, 2 * LANES), F32),
            pltpu.SemaphoreType.DMA((sets + 4,)),
        ],
        compiler_params=pltpu.CompilerParams(vmem_limit_bytes=limit),
        cost_estimate=pl.CostEstimate(flops=2 * 10**9, bytes_accessed=2 * MEBI, transcendentals=0),
        name="compress",
    )(*[pltpu.with_memory_space_constraint(x, pltpu.HBM) for x in (samples, rep, fwd, inv, twd)])


def doppler_kernel(x_ref, tab_ref, pow_ref, first_ref, second_ref, mid_ref, part_ref):
    channels = pow_ref.shape[0]
    sets = x_ref.shape[1] // (2 * ROWS)
    halves = sets // channels
    for i in range(sets):
        c, half = i // halves, i % halves

        def load(s, i=i):
            return tuple(x_ref[slot(s), i * 2 * ROWS + part * ROWS : i * 2 * ROWS + (part + 1) * ROWS, :] for part in range(2))

        def keep(j, value, i=i):
            mid_ref[i, 0, j], mid_ref[i, 1, j] = value

        def fetch(j, i=i):
            return (mid_ref[i, 0, j], mid_ref[i, 1, j])

        def store(k, value, c=c, half=half):
            tile, d1 = k // ROWS, k % ROWS
            for part in range(2):
                at = (d1 * 2 + part) * FINE + half * ROWS
                part_ref[tile, at : at + ROWS, c * LANES : (c + 1) * LANES] = value[part]

        fft32(load, keep, fetch, store, -1)
    scale = INPUT_SCALE * INPUT_SCALE / (float(RANGE) * float(RANGE) * PULSES)
    for tile in range(FAN // ROWS):
        high, low = split(part_ref[tile])
        out = dot(tab_ref[tile, 0], high) + dot(tab_ref[tile, 0], low) + dot(tab_ref[tile, 1], high)
        half = out.shape[0] // 2
        power = (out[:half] * out[:half] + out[half:] * out[half:]) * scale
        for d2 in range(FINE):
            for c in range(channels):
                at = d2 * FAN + tile * ROWS
                pow_ref[c, at : at + ROWS, :] = power[d2 * ROWS : (d2 + 1) * ROWS, c * LANES : (c + 1) * LANES]
    rows = PULSES // PACK
    lane = lax.broadcasted_iota(jnp.int32, (rows, LANES), 1)
    even = lax.broadcast(lax.rem(lax.axis_index("pulse"), 2), (rows, LANES)) == 0
    for c in range(channels):
        low_piece = high_piece = None
        for b in range(PACK):
            x = pow_ref[c, b * rows : (b + 1) * rows, :]
            low = pltpu.roll(x, b * PARTS, 1) if b else x
            shift = (b * PARTS - (LANES - PARTS)) % LANES
            high = pltpu.roll(x, shift, 1) if shift else x
            mine = lane >= b * PARTS
            low_piece = low if low_piece is None else jnp.where(mine, low, low_piece)
            high_piece = high if high_piece is None else jnp.where(mine, high, high_piece)
        first_ref[c * rows : (c + 1) * rows, :] = jnp.where(even, high_piece, low_piece)
        second_ref[c * rows : (c + 1) * rows, :] = jnp.where(even, low_piece, high_piece)


def doppler(received, channels, limit):
    sets = received.shape[1] // (2 * ROWS)
    vmem = pl.BlockSpec(memory_space=pltpu.VMEM)
    edge = pltpu.VMEM((channels * PULSES // PACK, LANES), F32)
    tables = jnp.asarray(doppler_tables())
    return pl.pallas_call(
        doppler_kernel,
        out_shape=(pltpu.VMEM((channels, PULSES, LANES), F32), edge, edge),
        in_specs=[vmem, vmem],
        out_specs=(vmem, vmem, vmem),
        scratch_shapes=[
            pltpu.VMEM((sets, 2, FAN, ROWS, LANES), F32),
            pltpu.VMEM((FAN // ROWS, 2 * FINE * ROWS, channels * LANES), F32),
        ],
        compiler_params=pltpu.CompilerParams(vmem_limit_bytes=limit),
        cost_estimate=pl.CostEstimate(flops=2 * 10**9, bytes_accessed=2 * MEBI, transcendentals=0),
        name="doppler",
    )(
        pltpu.with_memory_space_constraint(received, pltpu.VMEM),
        pltpu.with_memory_space_constraint(tables, pltpu.VMEM),
    )


def windows_kernel(groups, window_ref, thresh_ref, core_ref, side_ref, line_ref):
    channels = window_ref.shape[0]
    total = groups * LANES
    gate = lax.broadcasted_iota(jnp.int32, (ROWS, LANES), 1) + lax.axis_index("pulse") * LANES
    row_id = lax.broadcasted_iota(jnp.int32, (LANES, LANES), 0)
    col_id = lax.broadcasted_iota(jnp.int32, (LANES, LANES), 1)
    piece, inner = row_id // PARTS, row_id % PARTS
    odd = lax.rem(lax.axis_index("pulse"), 2)
    first = LANES - odd * (LANES + PARTS)
    second = odd * (LANES + PARTS) - PARTS
    core_ref[...] = jnp.zeros_like(core_ref)
    for c in range(channels):
        guard, train = window_ref[c, 0], window_ref[c, 1]
        reach = guard + train

        def band(offset, extra=True):
            distance = jnp.abs(offset)
            return jnp.where((distance > guard) & (distance <= reach) & extra, 1.0, 0.0).astype(BF16)

        core_ref[c * LANES : (c + 1) * LANES, c * LANES : (c + 1) * LANES] = band(row_id - col_id)
        for b in range(PACK):
            at = b * LANES
            side_ref[c, :LANES, at : at + LANES] = band(inner + first - col_id, piece == b)
            side_ref[c, LANES:, at : at + LANES] = band(inner + second - col_id, piece == b)
        ahead = total - 1 - gate
        cells = jnp.minimum(gate, reach) - jnp.minimum(gate, guard)
        cells = cells + jnp.minimum(ahead, reach) - jnp.minimum(ahead, guard)
        line_ref[c, 0] = cells.astype(F32)
        over = jnp.zeros((ROWS, LANES), F32) + thresh_ref[c, 1].astype(F32)
        line_ref[c, 1] = over / thresh_ref[c, 0].astype(F32)


def windows(window, thresh, groups, limit):
    channels = window.shape[0]
    vmem = pl.BlockSpec(memory_space=pltpu.VMEM)
    smem = pl.BlockSpec(memory_space=pltpu.SMEM)
    return pl.pallas_call(
        functools.partial(windows_kernel, groups),
        out_shape=(
            pltpu.VMEM((channels * LANES, channels * LANES), BF16),
            pltpu.VMEM((channels, 2 * LANES, PACK * LANES), BF16),
            pltpu.VMEM((channels, 2, ROWS, LANES), F32),
        ),
        in_specs=[smem, smem],
        out_specs=(vmem, vmem, vmem),
        compiler_params=pltpu.CompilerParams(vmem_limit_bytes=limit),
        cost_estimate=pl.CostEstimate(flops=10**7, bytes_accessed=MEBI, transcendentals=0),
        name="windows",
    )(window, thresh)


def core_kernel(pow_ref, band_ref, noise_ref):
    channels = pow_ref.shape[0]
    high, low = split(jnp.concatenate([pow_ref[c] for c in range(channels)], axis=1))
    noise = dot(high, band_ref[...]) + dot(low, band_ref[...])
    for c in range(channels):
        noise_ref[c] = noise[:, c * LANES : (c + 1) * LANES]


def core(power, band, limit):
    vmem = pl.BlockSpec(memory_space=pltpu.VMEM)
    return pl.pallas_call(
        core_kernel,
        out_shape=pltpu.VMEM(power.shape, F32),
        in_specs=[vmem, vmem],
        out_specs=vmem,
        compiler_params=pltpu.CompilerParams(vmem_limit_bytes=limit),
        cost_estimate=pl.CostEstimate(flops=2 * 10**9, bytes_accessed=MEBI, transcendentals=0),
        name="core",
    )(in_vmem(power), in_vmem(band))


def in_vmem(x):
    return pltpu.with_memory_space_constraint(x, pltpu.VMEM)


def cfar_kernel(pow_ref, noise_ref, first_ref, second_ref, side_ref, line_ref, out_hbm, soft_ref, ratio_ref, sems):
    channels = pow_ref.shape[0]
    stores = []
    rows = PULSES // PACK
    soft_sum = jnp.zeros((ROWS, LANES), F32)
    for c in range(channels):
        halo = jnp.concatenate([ref[c * rows : (c + 1) * rows, :] for ref in (first_ref, second_ref)], axis=1)
        high, low = split(halo)
        side = dot(high, side_ref[c]) + dot(low, side_ref[c])
        cells = jnp.concatenate([line_ref[c, 0]] * (rows // ROWS), axis=0)
        over = jnp.concatenate([line_ref[c, 1]] * (rows // ROWS), axis=0)
        for b in range(PACK):
            at = b * rows
            noise = noise_ref[c, at : at + rows, :] + side[:, b * LANES : (b + 1) * LANES]
            ratio = pow_ref[c, at : at + rows, :] * cells / (noise + EPSILON)
            ratio_ref[c, at : at + rows, :] = ratio
            piece = (c, pl.ds(at, rows))
            stores.append(pltpu.make_async_copy(ratio_ref.at[piece], out_hbm.at[piece], sems.at[len(stores)]))
            stores[-1].start()
            soft = jnp.clip(ratio * over - 1.0, 0.0, 1.0)
            soft_sum = soft_sum + soft.reshape(rows // ROWS, ROWS, LANES).sum(axis=0)
    soft_ref[...] = jnp.broadcast_to(jnp.sum(soft_sum, axis=0, keepdims=True), soft_ref.shape)
    for store in stores:
        store.wait()


def cfar(power, noise, first, second, side, line, peers, limit):
    vmem = pl.BlockSpec(memory_space=pltpu.VMEM)
    return pl.pallas_call(
        cfar_kernel,
        out_shape=(pltpu.HBM(power.shape, F32), pltpu.VMEM((peers, LANES), F32)),
        in_specs=[vmem] * 6,
        out_specs=(pl.BlockSpec(memory_space=pltpu.HBM), vmem),
        scratch_shapes=[
            pltpu.VMEM(power.shape, F32),
            pltpu.SemaphoreType.DMA((power.shape[0] * PACK,)),
        ],
        compiler_params=pltpu.CompilerParams(vmem_limit_bytes=limit),
        cost_estimate=pl.CostEstimate(flops=10**9, bytes_accessed=2 * MEBI, transcendentals=0),
        name="cfar",
    )(*[in_vmem(x) for x in (power, noise, first, second, side, line)])


def local(samples, replica, window, thresh):
    groups = lax.axis_size("pulse")
    channels = samples.shape[1]
    assert samples.shape[3] == RANGE and groups == FAN and samples.shape[2] == FINE
    limit = 24 * MEBI
    ready = compress(samples, replica, limit)
    received = lax.all_to_all(ready, "pulse", 0, 0, axis_index_groups=[ORDER])
    power, first, second = doppler(received, channels, limit)
    window, first = lax.optimization_barrier((window, first))
    band, side, line = windows(window, thresh, groups, limit)
    first = lax.ppermute(first, "pulse", [(i, i ^ 1) for i in range(groups)])
    second = lax.ppermute(second, "pulse", [(i, ((i + 1) ^ 1) - 1) for i in range(1, groups - 1)])
    noise = core(power, band, limit)
    peers = lax.axis_size("chan") * lax.axis_size("sub")
    ratio_map, soft = cfar(power, noise, first, second, side, line, peers, limit)
    near = [i ^ (peers // 2 + 1) for i in range(peers)]
    far = [(i + groups // 2) % groups for i in range(groups)]
    soft = soft.reshape(peers, 1, LANES)
    plane = jnp.sum(lax.all_to_all(soft, ("chan", "sub"), 0, 0, axis_index_groups=[near]), axis=0, keepdims=True)
    counts = lax.all_to_all(jnp.broadcast_to(plane, (groups, 1, LANES)), "pulse", 0, 0, axis_index_groups=[far])
    detections = jnp.sum(counts) * (1024.0 / (PULSES * RANGE))
    return (ratio_map, detections.reshape(1))


def solution(mesh):
    in_specs = (
        P(None, ("grp", "chan", "sub"), "pulse", None),
        P(),
        P(("grp", "chan", "sub"), None),
        P(("grp", "chan", "sub"), None),
    )
    out_specs = (P(("grp", "chan", "sub"), None, "pulse"), P("grp"))
    return jax.shard_map(local, mesh=mesh, in_specs=in_specs, out_specs=out_specs, check_vma=False)
```

```python
import functools
import math

import jax
import jax.numpy as jnp
import numpy as np
from jax import lax
from jax.experimental import pallas as pl
from jax.experimental.pallas import tpu as pltpu
from jax.sharding import PartitionSpec as P

PULSES = 512
RANGE = 4096
GUARD_MAX = 4
TRAIN_MAX = 28

EPSILON = 1e-06
INPUT_SCALE = 1.0 / 2048.0
MARGIN = GUARD_MAX + TRAIN_MAX

LANES = 128
ROWS = 8
FAN = 32
TAIL = RANGE // FAN
FINE = PULSES // FAN
PARTS = MARGIN
PACK = LANES // PARTS
F32 = jnp.float32
BF16 = jnp.bfloat16
MEBI = 1 << 20
ORDER = [0, 1, 31, 2, 6, 7, 5, 4, 12, 13, 10, 14, 15, 11, 9, 8, 24, 25, 27, 26, 30, 28, 29, 3, 20, 21, 23, 22, 18, 19, 17, 16]


def slot(device):
    return ORDER.index(device)


def split_table(table):
    high = table.astype(BF16)
    low = (table - high.astype(np.float64)).astype(BF16)
    return np.stack([high, low])


def unit(product, period):
    angle = 2.0 * np.pi / period * (np.asarray(product, np.int64) % period)
    return np.cos(angle), np.sin(angle)


def range_tables():
    b = np.arange(TAIL)[:, None]
    col = np.arange(TAIL)[None, :]
    freq = 4 * (col % FAN) + col // FAN
    cos, sin = unit(b * freq, TAIL)
    forward = np.block([[cos, -sin], [sin, cos]])
    inverse = forward.T
    k1 = np.arange(FAN)[:, None]
    cos, sin = unit(k1 * np.arange(TAIL)[None, :], RANGE)
    twiddle = np.stack([cos, sin]).astype(np.float32)
    return split_table(forward), split_table(inverse), twiddle


def doppler_tables():
    tiles = []
    for t in range(FAN // ROWS):
        table = np.zeros((2, FINE, ROWS, ROWS, 2, FINE))
        for d1 in range(ROWS):
            bins = 8 * t + d1 + FAN * np.arange(FINE)[:, None]
            cos, sin = unit(bins * np.arange(FINE)[None, :], PULSES)
            table[0, :, d1, d1, 0] = cos
            table[0, :, d1, d1, 1] = sin
            table[1, :, d1, d1, 0] = -sin
            table[1, :, d1, d1, 1] = cos
        tiles.append(split_table(table.reshape(2 * PULSES // 4, 2 * PULSES // 4)))
    return np.stack(tiles)


def add(x, y):
    return (x[0] + y[0], x[1] + y[1])


def sub(x, y):
    return (x[0] - y[0], x[1] - y[1])


def turn(x, sign):
    return (-x[1], x[0]) if sign > 0 else (x[1], -x[0])


def add_turn(x, y, sign):
    if sign > 0:
        return (x[0] - y[1], x[1] + y[0])
    return (x[0] + y[1], x[1] - y[0])


def by_constant(x, index, period, sign):
    index = index % period
    if index == 0:
        return x
    angle = 2.0 * math.pi * index / period
    cos, sin = math.cos(angle), sign * math.sin(angle)
    if 8 * index == period:
        return ((x[0] - x[1]) * cos, (x[0] + x[1]) * cos) if sign > 0 else ((x[0] + x[1]) * cos, (x[1] - x[0]) * cos)
    if 4 * index == period:
        return turn(x, sign)
    return (x[0] * cos - x[1] * sin, x[0] * sin + x[1] * cos)


def fft4(x, sign):
    a, b = add(x[0], x[2]), sub(x[0], x[2])
    c, d = add(x[1], x[3]), sub(x[1], x[3])
    return [add(a, c), add_turn(b, d, sign), sub(a, c), add_turn(b, d, -sign)]


def fft8(x, sign):
    even, odd = fft4(x[0::2], sign), fft4(x[1::2], sign)
    root = math.sqrt(0.5)
    out = [None] * 8
    out[0], out[4] = add(even[0], odd[0]), sub(even[0], odd[0])
    out[2], out[6] = add_turn(even[2], odd[2], sign), add_turn(even[2], odd[2], -sign)
    for k in (1, 3):
        o = odd[k]
        if k == 1:
            w = (o[0] - o[1], o[0] + o[1]) if sign > 0 else (o[0] + o[1], o[1] - o[0])
        else:
            w = (-o[0] - o[1], o[0] - o[1]) if sign > 0 else (o[1] - o[0], -o[0] - o[1])
        w = (w[0] * root, w[1] * root)
        out[k], out[k + 4] = add(even[k], w), sub(even[k], w)
    return out


def fft32(load, keep, fetch, store, sign):
    for n2 in range(8):
        mid = fft4([load(n2 + 8 * n1) for n1 in range(4)], sign)
        for k1 in range(4):
            keep(k1 * 8 + n2, by_constant(mid[k1], n2 * k1, 32, sign))
    for k1 in range(4):
        out = fft8([fetch(k1 * 8 + n2) for n2 in range(8)], sign)
        for k2 in range(8):
            store(k1 + 4 * k2, out[k2])


def split(x):
    high = x.astype(BF16)
    return high, (x - high.astype(F32)).astype(BF16)


def dot(x, y):
    return jnp.dot(x, y, preferred_element_type=F32)


def compress_kernel(
    x_hbm, rep_hbm, fwd_hbm, inv_hbm, twd_hbm, o_ref,
    x_ref, rep_ref, fwd_ref, inv_ref, twd_ref, h_ref, mid_ref, high_ref, low_ref, out_ref, sems,
):
    channels, pulses = x_hbm.shape[1], x_hbm.shape[2]
    sets = [(c, p) for c in range(channels) for p in range(0, pulses, ROWS)]
    loads = [
        pltpu.make_async_copy(x_hbm.at[:, c, pl.ds(p, ROWS)], x_ref.at[i], sems.at[i]) for i, (c, p) in enumerate(sets)
    ]
    n = len(sets)
    load_rep = pltpu.make_async_copy(rep_hbm, rep_ref, sems.at[n])
    load_twd = pltpu.make_async_copy(twd_hbm, twd_ref, sems.at[n + 1])
    load_fwd = pltpu.make_async_copy(fwd_hbm, fwd_ref, sems.at[n + 2])
    load_inv = pltpu.make_async_copy(inv_hbm, inv_ref, sems.at[n + 3])
    for load in [loads[0], load_rep, load_twd, load_fwd, *loads[1:], load_inv]:
        load.start()

    load_rep.wait()
    for part in range(2):
        turned = rep_ref[pl.ds(part, FAN, stride=2), :].T
        h_ref[part] = jnp.concatenate([turned[q * FAN : (q + 1) * FAN] for q in range(4)], axis=1)
    load_twd.wait()

    def row(ref, part, k):
        return jnp.broadcast_to(ref[part, k : k + 1, :], (ROWS, LANES))

    def put(i, k, value):
        at = (i * FAN + k) * ROWS
        for part in range(2):
            high, low = split(value[part])
            high_ref[at : at + ROWS, part * LANES : (part + 1) * LANES] = high
            low_ref[at : at + ROWS, part * LANES : (part + 1) * LANES] = low

    def product(table):
        for t in range(4):
            at = pl.ds(t * 256, 256)
            high = high_ref[at]
            out_ref[at] = dot(high, table[0]) + dot(low_ref[at], table[0]) + dot(high, table[1])

    for i in range(n):
        loads[i].wait()

        def load(a, i=i):
            return tuple(x_ref[i, part, :, a * LANES : (a + 1) * LANES].astype(F32) for part in range(2))

        def keep(j, value, i=i):
            mid_ref[i, 0, j], mid_ref[i, 1, j] = value

        def fetch(j, i=i):
            return (mid_ref[i, 0, j], mid_ref[i, 1, j])

        def twisted(k, value, i=i):
            cos, sin = row(twd_ref, 0, k), row(twd_ref, 1, k)
            put(i, k, (value[0] * cos + value[1] * sin, value[1] * cos - value[0] * sin))

        fft32(load, keep, fetch, twisted, -1)
    load_fwd.wait()
    product(fwd_ref)
    for i in range(n):
        for k in range(FAN):
            at = (i * FAN + k) * ROWS
            re, im = out_ref[at : at + ROWS, :LANES], out_ref[at : at + ROWS, LANES:]
            h_re, h_im = row(h_ref, 0, k), row(h_ref, 1, k)
            put(i, k, (re * h_re - im * h_im, re * h_im + im * h_re))
    load_inv.wait()
    product(inv_ref)
    for i in range(n):

        def keep(j, value, i=i):
            mid_ref[i, 0, j], mid_ref[i, 1, j] = value

        def fetch(j, i=i):
            return (mid_ref[i, 0, j], mid_ref[i, 1, j])

        def untwisted(k, i=i):
            at = (i * FAN + k) * ROWS
            re, im = out_ref[at : at + ROWS, :LANES], out_ref[at : at + ROWS, LANES:]
            cos, sin = row(twd_ref, 0, k), row(twd_ref, 1, k)
            return (re * cos - im * sin, im * cos + re * sin)

        def store(a, value, i=i):
            for part in range(2):
                o_ref[slot(a), i * 2 * ROWS + part * ROWS : i * 2 * ROWS + (part + 1) * ROWS, :] = value[part]

        fft32(untwisted, keep, fetch, store, 1)


def compress(samples, replica, limit):
    fwd, inv, twd = [jnp.asarray(table) for table in range_tables()]
    sets = samples.shape[1] * samples.shape[2] // ROWS
    rep = replica.reshape(2, FAN, LANES).transpose(1, 0, 2).reshape(2 * FAN, LANES)
    any_space = pl.BlockSpec(memory_space=pltpu.HBM)
    return pl.pallas_call(
        compress_kernel,
        out_shape=pltpu.VMEM((FAN, sets * 2 * ROWS, LANES), F32),
        in_specs=[any_space] * 5,
        out_specs=pl.BlockSpec(memory_space=pltpu.VMEM),
        scratch_shapes=[
            pltpu.VMEM((sets, 2, ROWS, RANGE), jnp.int32),
            pltpu.VMEM((2 * FAN, LANES), F32),
            pltpu.VMEM((2, 2 * TAIL, 2 * TAIL), BF16),
            pltpu.VMEM((2, 2 * TAIL, 2 * TAIL), BF16),
            pltpu.VMEM((2, FAN, LANES), F32),
            pltpu.VMEM((2, FAN, LANES), F32),
            pltpu.VMEM((sets, 2, FAN, ROWS, LANES), F32),
            pltpu.VMEM((sets * FAN * ROWS, 2 * LANES), BF16),
            pltpu.VMEM((sets * FAN * ROWS, 2 * LANES), BF16),
            pltpu.VMEM((sets * FAN * ROWS, 2 * LANES), F32),
            pltpu.SemaphoreType.DMA((sets + 4,)),
        ],
        compiler_params=pltpu.CompilerParams(vmem_limit_bytes=limit),
        cost_estimate=pl.CostEstimate(flops=2 * 10**9, bytes_accessed=2 * MEBI, transcendentals=0),
        name="compress",
    )(*[pltpu.with_memory_space_constraint(x, pltpu.HBM) for x in (samples, rep, fwd, inv, twd)])


def doppler_kernel(x_ref, tab_ref, pow_ref, first_ref, second_ref, mid_ref, part_ref):
    channels = pow_ref.shape[0]
    sets = x_ref.shape[1] // (2 * ROWS)
    halves = sets // channels
    for i in range(sets):
        c, half = i // halves, i % halves

        def load(s, i=i):
            return tuple(x_ref[slot(s), i * 2 * ROWS + part * ROWS : i * 2 * ROWS + (part + 1) * ROWS, :] for part in range(2))

        def keep(j, value, i=i):
            mid_ref[i, 0, j], mid_ref[i, 1, j] = value

        def fetch(j, i=i):
            return (mid_ref[i, 0, j], mid_ref[i, 1, j])

        def store(k, value, c=c, half=half):
            tile, d1 = k // ROWS, k % ROWS
            for part in range(2):
                at = (d1 * 2 + part) * FINE + half * ROWS
                part_ref[tile, at : at + ROWS, c * LANES : (c + 1) * LANES] = value[part]

        fft32(load, keep, fetch, store, -1)
    scale = INPUT_SCALE * INPUT_SCALE / (float(RANGE) * float(RANGE) * PULSES)
    for tile in range(FAN // ROWS):
        high, low = split(part_ref[tile])
        out = dot(tab_ref[tile, 0], high) + dot(tab_ref[tile, 0], low) + dot(tab_ref[tile, 1], high)
        half = out.shape[0] // 2
        power = (out[:half] * out[:half] + out[half:] * out[half:]) * scale
        for d2 in range(FINE):
            for c in range(channels):
                at = d2 * FAN + tile * ROWS
                pow_ref[c, at : at + ROWS, :] = power[d2 * ROWS : (d2 + 1) * ROWS, c * LANES : (c + 1) * LANES]
    rows = PULSES // PACK
    lane = lax.broadcasted_iota(jnp.int32, (rows, LANES), 1)
    even = lax.broadcast(lax.rem(lax.axis_index("pulse"), 2), (rows, LANES)) == 0
    for c in range(channels):
        low_piece = high_piece = None
        for b in range(PACK):
            x = pow_ref[c, b * rows : (b + 1) * rows, :]
            low = pltpu.roll(x, b * PARTS, 1) if b else x
            shift = (b * PARTS - (LANES - PARTS)) % LANES
            high = pltpu.roll(x, shift, 1) if shift else x
            mine = lane >= b * PARTS
            low_piece = low if low_piece is None else jnp.where(mine, low, low_piece)
            high_piece = high if high_piece is None else jnp.where(mine, high, high_piece)
        first_ref[c * rows : (c + 1) * rows, :] = jnp.where(even, high_piece, low_piece)
        second_ref[c * rows : (c + 1) * rows, :] = jnp.where(even, low_piece, high_piece)


def doppler(received, channels, limit):
    sets = received.shape[1] // (2 * ROWS)
    vmem = pl.BlockSpec(memory_space=pltpu.VMEM)
    edge = pltpu.VMEM((channels * PULSES // PACK, LANES), F32)
    tables = jnp.asarray(doppler_tables())
    return pl.pallas_call(
        doppler_kernel,
        out_shape=(pltpu.VMEM((channels, PULSES, LANES), F32), edge, edge),
        in_specs=[vmem, vmem],
        out_specs=(vmem, vmem, vmem),
        scratch_shapes=[
            pltpu.VMEM((sets, 2, FAN, ROWS, LANES), F32),
            pltpu.VMEM((FAN // ROWS, 2 * FINE * ROWS, channels * LANES), F32),
        ],
        compiler_params=pltpu.CompilerParams(vmem_limit_bytes=limit),
        cost_estimate=pl.CostEstimate(flops=2 * 10**9, bytes_accessed=2 * MEBI, transcendentals=0),
        name="doppler",
    )(
        pltpu.with_memory_space_constraint(received, pltpu.VMEM),
        pltpu.with_memory_space_constraint(tables, pltpu.VMEM),
    )


def windows_kernel(groups, window_ref, thresh_ref, core_ref, side_ref, line_ref):
    channels = window_ref.shape[0]
    total = groups * LANES
    gate = lax.broadcasted_iota(jnp.int32, (ROWS, LANES), 1) + lax.axis_index("pulse") * LANES
    row_id = lax.broadcasted_iota(jnp.int32, (LANES, LANES), 0)
    col_id = lax.broadcasted_iota(jnp.int32, (LANES, LANES), 1)
    piece, inner = row_id // PARTS, row_id % PARTS
    odd = lax.rem(lax.axis_index("pulse"), 2)
    first = LANES - odd * (LANES + PARTS)
    second = odd * (LANES + PARTS) - PARTS
    core_ref[...] = jnp.zeros_like(core_ref)
    for c in range(channels):
        guard, train = window_ref[c, 0], window_ref[c, 1]
        reach = guard + train

        def band(offset, extra=True):
            distance = jnp.abs(offset)
            return jnp.where((distance > guard) & (distance <= reach) & extra, 1.0, 0.0).astype(BF16)

        core_ref[c * LANES : (c + 1) * LANES, c * LANES : (c + 1) * LANES] = band(row_id - col_id)
        for b in range(PACK):
            at = b * LANES
            side_ref[c, :LANES, at : at + LANES] = band(inner + first - col_id, piece == b)
            side_ref[c, LANES:, at : at + LANES] = band(inner + second - col_id, piece == b)
        ahead = total - 1 - gate
        cells = jnp.minimum(gate, reach) - jnp.minimum(gate, guard)
        cells = cells + jnp.minimum(ahead, reach) - jnp.minimum(ahead, guard)
        line_ref[c, 0] = cells.astype(F32)
        over = jnp.zeros((ROWS, LANES), F32) + thresh_ref[c, 1].astype(F32)
        line_ref[c, 1] = over / thresh_ref[c, 0].astype(F32)


def windows(window, thresh, groups, limit):
    channels = window.shape[0]
    vmem = pl.BlockSpec(memory_space=pltpu.VMEM)
    smem = pl.BlockSpec(memory_space=pltpu.SMEM)
    return pl.pallas_call(
        functools.partial(windows_kernel, groups),
        out_shape=(
            pltpu.VMEM((channels * LANES, channels * LANES), BF16),
            pltpu.VMEM((channels, 2 * LANES, PACK * LANES), BF16),
            pltpu.VMEM((channels, 2, ROWS, LANES), F32),
        ),
        in_specs=[smem, smem],
        out_specs=(vmem, vmem, vmem),
        compiler_params=pltpu.CompilerParams(vmem_limit_bytes=limit),
        cost_estimate=pl.CostEstimate(flops=10**7, bytes_accessed=MEBI, transcendentals=0),
        name="windows",
    )(window, thresh)


def core_kernel(pow_ref, band_ref, noise_ref):
    channels = pow_ref.shape[0]
    high, low = split(jnp.concatenate([pow_ref[c] for c in range(channels)], axis=1))
    noise = dot(high, band_ref[...]) + dot(low, band_ref[...])
    for c in range(channels):
        noise_ref[c] = noise[:, c * LANES : (c + 1) * LANES]


def core(power, band, limit):
    vmem = pl.BlockSpec(memory_space=pltpu.VMEM)
    return pl.pallas_call(
        core_kernel,
        out_shape=pltpu.VMEM(power.shape, F32),
        in_specs=[vmem, vmem],
        out_specs=vmem,
        compiler_params=pltpu.CompilerParams(vmem_limit_bytes=limit),
        cost_estimate=pl.CostEstimate(flops=2 * 10**9, bytes_accessed=MEBI, transcendentals=0),
        name="core",
    )(in_vmem(power), in_vmem(band))


def in_vmem(x):
    return pltpu.with_memory_space_constraint(x, pltpu.VMEM)


def cfar_kernel(pow_ref, noise_ref, first_ref, second_ref, side_ref, line_ref, out_hbm, soft_ref, ratio_ref, sems):
    channels = pow_ref.shape[0]
    stores = []
    rows = PULSES // PACK
    soft_sum = jnp.zeros((ROWS, LANES), F32)
    for c in range(channels):
        halo = jnp.concatenate([ref[c * rows : (c + 1) * rows, :] for ref in (first_ref, second_ref)], axis=1)
        high, low = split(halo)
        side = dot(high, side_ref[c]) + dot(low, side_ref[c])
        cells = jnp.concatenate([line_ref[c, 0]] * (rows // ROWS), axis=0)
        over = jnp.concatenate([line_ref[c, 1]] * (rows // ROWS), axis=0)
        for b in range(PACK):
            at = b * rows
            noise = noise_ref[c, at : at + rows, :] + side[:, b * LANES : (b + 1) * LANES]
            ratio = pow_ref[c, at : at + rows, :] * cells / (noise + EPSILON)
            ratio_ref[c, at : at + rows, :] = ratio
            piece = (c, pl.ds(at, rows))
            stores.append(pltpu.make_async_copy(ratio_ref.at[piece], out_hbm.at[piece], sems.at[len(stores)]))
            stores[-1].start()
            soft = jnp.clip(ratio * over - 1.0, 0.0, 1.0)
            soft_sum = soft_sum + soft.reshape(rows // ROWS, ROWS, LANES).sum(axis=0)
    count = jnp.sum(soft_sum, axis=0, keepdims=True) * (1024.0 / (PULSES * RANGE))
    soft_ref[...] = jnp.broadcast_to(count, soft_ref.shape)
    for store in stores:
        store.wait()


def cfar(power, noise, first, second, side, line, peers, limit):
    vmem = pl.BlockSpec(memory_space=pltpu.VMEM)
    return pl.pallas_call(
        cfar_kernel,
        out_shape=(pltpu.HBM(power.shape, F32), pltpu.VMEM((peers, LANES), F32)),
        in_specs=[vmem] * 6,
        out_specs=(pl.BlockSpec(memory_space=pltpu.HBM), vmem),
        scratch_shapes=[
            pltpu.VMEM(power.shape, F32),
            pltpu.SemaphoreType.DMA((power.shape[0] * PACK,)),
        ],
        compiler_params=pltpu.CompilerParams(vmem_limit_bytes=limit),
        cost_estimate=pl.CostEstimate(flops=10**9, bytes_accessed=2 * MEBI, transcendentals=0),
        name="cfar",
    )(*[in_vmem(x) for x in (power, noise, first, second, side, line)])


def local(samples, replica, window, thresh):
    groups = lax.axis_size("pulse")
    channels = samples.shape[1]
    assert samples.shape[3] == RANGE and groups == FAN and samples.shape[2] == FINE
    limit = 24 * MEBI
    ready = compress(samples, replica, limit)
    received = lax.all_to_all(ready, "pulse", 0, 0, axis_index_groups=[ORDER])
    power, first, second = doppler(received, channels, limit)
    window, first = lax.optimization_barrier((window, first))
    band, side, line = windows(window, thresh, groups, limit)
    first = lax.ppermute(first, "pulse", [(i, i ^ 1) for i in range(groups)])
    second = lax.ppermute(second, "pulse", [(i, ((i + 1) ^ 1) - 1) for i in range(1, groups - 1)])
    noise = core(power, band, limit)
    peers = lax.axis_size("chan") * lax.axis_size("sub")
    ratio_map, soft = cfar(power, noise, first, second, side, line, peers, limit)
    near = [i ^ (peers // 2 + 1) for i in range(peers)]
    far = [(i + groups // 2) % groups for i in range(groups)]
    soft = soft.reshape(peers, 1, LANES)
    plane = jnp.sum(lax.all_to_all(soft, ("chan", "sub"), 0, 0, axis_index_groups=[near]), axis=0, keepdims=True)
    counts = lax.all_to_all(jnp.broadcast_to(plane, (groups, 1, LANES)), "pulse", 0, 0, axis_index_groups=[far])
    detections = jnp.sum(counts)
    return (ratio_map, detections.reshape(1))


def solution(mesh):
    in_specs = (
        P(None, ("grp", "chan", "sub"), "pulse", None),
        P(),
        P(("grp", "chan", "sub"), None),
        P(("grp", "chan", "sub"), None),
    )
    out_specs = (P(("grp", "chan", "sub"), None, "pulse"), P("grp"))
    return jax.shard_map(local, mesh=mesh, in_specs=in_specs, out_specs=out_specs, check_vma=False)
```

```python
import functools
import math

import jax
import jax.numpy as jnp
import numpy as np
from jax import lax
from jax.experimental import pallas as pl
from jax.experimental.pallas import tpu as pltpu
from jax.sharding import PartitionSpec as P

PULSES = 512
RANGE = 4096
GUARD_MAX = 4
TRAIN_MAX = 28

EPSILON = 1e-06
INPUT_SCALE = 1.0 / 2048.0
MARGIN = GUARD_MAX + TRAIN_MAX

LANES = 128
ROWS = 8
FAN = 32
TAIL = RANGE // FAN
FINE = PULSES // FAN
PARTS = MARGIN
PACK = LANES // PARTS
F32 = jnp.float32
BF16 = jnp.bfloat16
MEBI = 1 << 20
ORDER = [0, 1, 31, 2, 6, 7, 5, 4, 12, 13, 10, 14, 15, 11, 9, 8, 24, 25, 27, 26, 30, 28, 29, 3, 20, 21, 23, 22, 18, 19, 17, 16]


def slot(device):
    return ORDER.index(device)


def split_table(table):
    high = table.astype(BF16)
    low = (table - high.astype(np.float64)).astype(BF16)
    return np.stack([high, low])


def unit(product, period):
    angle = 2.0 * np.pi / period * (np.asarray(product, np.int64) % period)
    return np.cos(angle), np.sin(angle)


def range_tables():
    b = np.arange(TAIL)[:, None]
    col = np.arange(TAIL)[None, :]
    freq = 4 * (col % FAN) + col // FAN
    cos, sin = unit(b * freq, TAIL)
    forward = np.block([[cos, -sin], [sin, cos]])
    inverse = forward.T
    k1 = np.arange(FAN)[:, None]
    cos, sin = unit(k1 * np.arange(TAIL)[None, :], RANGE)
    twiddle = np.stack([cos, sin]).astype(np.float32)
    return split_table(forward), split_table(inverse), twiddle


def doppler_tables():
    tiles = []
    for t in range(FAN // ROWS):
        table = np.zeros((2, FINE, ROWS, ROWS, 2, FINE))
        for d1 in range(ROWS):
            bins = 8 * t + d1 + FAN * np.arange(FINE)[:, None]
            cos, sin = unit(bins * np.arange(FINE)[None, :], PULSES)
            table[0, :, d1, d1, 0] = cos
            table[0, :, d1, d1, 1] = sin
            table[1, :, d1, d1, 0] = -sin
            table[1, :, d1, d1, 1] = cos
        tiles.append(split_table(table.reshape(2 * PULSES // 4, 2 * PULSES // 4)))
    return np.stack(tiles)


def add(x, y):
    return (x[0] + y[0], x[1] + y[1])


def sub(x, y):
    return (x[0] - y[0], x[1] - y[1])


def turn(x, sign):
    return (-x[1], x[0]) if sign > 0 else (x[1], -x[0])


def add_turn(x, y, sign):
    if sign > 0:
        return (x[0] - y[1], x[1] + y[0])
    return (x[0] + y[1], x[1] - y[0])


def by_constant(x, index, period, sign):
    index = index % period
    if index == 0:
        return x
    angle = 2.0 * math.pi * index / period
    cos, sin = math.cos(angle), sign * math.sin(angle)
    if 8 * index == period:
        return ((x[0] - x[1]) * cos, (x[0] + x[1]) * cos) if sign > 0 else ((x[0] + x[1]) * cos, (x[1] - x[0]) * cos)
    if 4 * index == period:
        return turn(x, sign)
    return (x[0] * cos - x[1] * sin, x[0] * sin + x[1] * cos)


def fft4(x, sign):
    a, b = add(x[0], x[2]), sub(x[0], x[2])
    c, d = add(x[1], x[3]), sub(x[1], x[3])
    return [add(a, c), add_turn(b, d, sign), sub(a, c), add_turn(b, d, -sign)]


def fft8(x, sign):
    even, odd = fft4(x[0::2], sign), fft4(x[1::2], sign)
    root = math.sqrt(0.5)
    out = [None] * 8
    out[0], out[4] = add(even[0], odd[0]), sub(even[0], odd[0])
    out[2], out[6] = add_turn(even[2], odd[2], sign), add_turn(even[2], odd[2], -sign)
    for k in (1, 3):
        o = odd[k]
        if k == 1:
            w = (o[0] - o[1], o[0] + o[1]) if sign > 0 else (o[0] + o[1], o[1] - o[0])
        else:
            w = (-o[0] - o[1], o[0] - o[1]) if sign > 0 else (o[1] - o[0], -o[0] - o[1])
        w = (w[0] * root, w[1] * root)
        out[k], out[k + 4] = add(even[k], w), sub(even[k], w)
    return out


def fft32(load, keep, fetch, store, sign):
    for n2 in range(8):
        mid = fft4([load(n2 + 8 * n1) for n1 in range(4)], sign)
        for k1 in range(4):
            keep(k1 * 8 + n2, by_constant(mid[k1], n2 * k1, 32, sign))
    for k1 in range(4):
        out = fft8([fetch(k1 * 8 + n2) for n2 in range(8)], sign)
        for k2 in range(8):
            store(k1 + 4 * k2, out[k2])


def split(x):
    high = x.astype(BF16)
    return high, (x - high.astype(F32)).astype(BF16)


def dot(x, y):
    return jnp.dot(x, y, preferred_element_type=F32)


def compress_kernel(
    x_hbm, rep_hbm, fwd_hbm, inv_hbm, twd_hbm, o_ref,
    x_ref, rep_ref, fwd_ref, inv_ref, twd_ref, h_ref, mid_ref, high_ref, low_ref, out_ref, sems,
):
    channels, pulses = x_hbm.shape[1], x_hbm.shape[2]
    sets = [(c, p) for c in range(channels) for p in range(0, pulses, ROWS)]
    loads = [
        pltpu.make_async_copy(x_hbm.at[:, c, pl.ds(p, ROWS)], x_ref.at[i], sems.at[i]) for i, (c, p) in enumerate(sets)
    ]
    n = len(sets)
    load_rep = pltpu.make_async_copy(rep_hbm, rep_ref, sems.at[n])
    load_twd = pltpu.make_async_copy(twd_hbm, twd_ref, sems.at[n + 1])
    load_fwd = pltpu.make_async_copy(fwd_hbm, fwd_ref, sems.at[n + 2])
    load_inv = pltpu.make_async_copy(inv_hbm, inv_ref, sems.at[n + 3])
    for load in [loads[0], load_rep, load_twd, load_fwd, *loads[1:], load_inv]:
        load.start()

    load_rep.wait()
    for part in range(2):
        turned = rep_ref[pl.ds(part, FAN, stride=2), :].T
        h_ref[part] = jnp.concatenate([turned[q * FAN : (q + 1) * FAN] for q in range(4)], axis=1)
    load_twd.wait()

    def row(ref, part, k):
        return jnp.broadcast_to(ref[part, k : k + 1, :], (ROWS, LANES))

    def put(i, k, value):
        at = (i * FAN + k) * ROWS
        for part in range(2):
            high, low = split(value[part])
            high_ref[at : at + ROWS, part * LANES : (part + 1) * LANES] = high
            low_ref[at : at + ROWS, part * LANES : (part + 1) * LANES] = low

    def product(table):
        for t in range(4):
            at = pl.ds(t * 256, 256)
            high = high_ref[at]
            out_ref[at] = dot(high, table[0]) + dot(low_ref[at], table[0]) + dot(high, table[1])

    for i in range(n):
        loads[i].wait()

        def load(a, i=i):
            return tuple(x_ref[i, part, :, a * LANES : (a + 1) * LANES].astype(F32) for part in range(2))

        def keep(j, value, i=i):
            mid_ref[i, 0, j], mid_ref[i, 1, j] = value

        def fetch(j, i=i):
            return (mid_ref[i, 0, j], mid_ref[i, 1, j])

        def twisted(k, value, i=i):
            cos, sin = row(twd_ref, 0, k), row(twd_ref, 1, k)
            put(i, k, (value[0] * cos + value[1] * sin, value[1] * cos - value[0] * sin))

        fft32(load, keep, fetch, twisted, -1)
    load_fwd.wait()
    product(fwd_ref)
    for i in range(n):
        for k in range(FAN):
            at = (i * FAN + k) * ROWS
            re, im = out_ref[at : at + ROWS, :LANES], out_ref[at : at + ROWS, LANES:]
            h_re, h_im = row(h_ref, 0, k), row(h_ref, 1, k)
            put(i, k, (re * h_re - im * h_im, re * h_im + im * h_re))
    load_inv.wait()
    product(inv_ref)
    for i in range(n):

        def keep(j, value, i=i):
            mid_ref[i, 0, j], mid_ref[i, 1, j] = value

        def fetch(j, i=i):
            return (mid_ref[i, 0, j], mid_ref[i, 1, j])

        def untwisted(k, i=i):
            at = (i * FAN + k) * ROWS
            re, im = out_ref[at : at + ROWS, :LANES], out_ref[at : at + ROWS, LANES:]
            cos, sin = row(twd_ref, 0, k), row(twd_ref, 1, k)
            return (re * cos - im * sin, im * cos + re * sin)

        def store(a, value, i=i):
            for part in range(2):
                o_ref[slot(a), i * 2 * ROWS + part * ROWS : i * 2 * ROWS + (part + 1) * ROWS, :] = value[part]

        fft32(untwisted, keep, fetch, store, 1)


def compress(samples, replica, limit):
    fwd, inv, twd = [jnp.asarray(table) for table in range_tables()]
    sets = samples.shape[1] * samples.shape[2] // ROWS
    rep = replica.reshape(2, FAN, LANES).transpose(1, 0, 2).reshape(2 * FAN, LANES)
    any_space = pl.BlockSpec(memory_space=pltpu.HBM)
    return pl.pallas_call(
        compress_kernel,
        out_shape=pltpu.VMEM((FAN, sets * 2 * ROWS, LANES), F32),
        in_specs=[any_space] * 5,
        out_specs=pl.BlockSpec(memory_space=pltpu.VMEM),
        scratch_shapes=[
            pltpu.VMEM((sets, 2, ROWS, RANGE), jnp.int32),
            pltpu.VMEM((2 * FAN, LANES), F32),
            pltpu.VMEM((2, 2 * TAIL, 2 * TAIL), BF16),
            pltpu.VMEM((2, 2 * TAIL, 2 * TAIL), BF16),
            pltpu.VMEM((2, FAN, LANES), F32),
            pltpu.VMEM((2, FAN, LANES), F32),
            pltpu.VMEM((sets, 2, FAN, ROWS, LANES), F32),
            pltpu.VMEM((sets * FAN * ROWS, 2 * LANES), BF16),
            pltpu.VMEM((sets * FAN * ROWS, 2 * LANES), BF16),
            pltpu.VMEM((sets * FAN * ROWS, 2 * LANES), F32),
            pltpu.SemaphoreType.DMA((sets + 4,)),
        ],
        compiler_params=pltpu.CompilerParams(vmem_limit_bytes=limit),
        cost_estimate=pl.CostEstimate(flops=2 * 10**9, bytes_accessed=2 * MEBI, transcendentals=0),
        name="compress",
    )(*[pltpu.with_memory_space_constraint(x, pltpu.HBM) for x in (samples, rep, fwd, inv, twd)])


def doppler_kernel(x_ref, tab_ref, pow_ref, first_ref, second_ref, mid_ref, part_ref):
    channels = pow_ref.shape[0]
    sets = x_ref.shape[1] // (2 * ROWS)
    halves = sets // channels
    for i in range(sets):
        c, half = i // halves, i % halves

        def load(s, i=i):
            return tuple(x_ref[slot(s), i * 2 * ROWS + part * ROWS : i * 2 * ROWS + (part + 1) * ROWS, :] for part in range(2))

        def keep(j, value, i=i):
            mid_ref[i, 0, j], mid_ref[i, 1, j] = value

        def fetch(j, i=i):
            return (mid_ref[i, 0, j], mid_ref[i, 1, j])

        def store(k, value, c=c, half=half):
            tile, d1 = k // ROWS, k % ROWS
            for part in range(2):
                at = (d1 * 2 + part) * FINE + half * ROWS
                part_ref[tile, at : at + ROWS, c * LANES : (c + 1) * LANES] = value[part]

        fft32(load, keep, fetch, store, -1)
    scale = INPUT_SCALE * INPUT_SCALE / (float(RANGE) * float(RANGE) * PULSES)
    lane = lax.broadcasted_iota(jnp.int32, (ROWS, LANES), 1)
    even = lax.broadcast(lax.rem(lax.axis_index("pulse"), 2), (ROWS, LANES)) == 0
    step = FINE // PACK
    for tile in range(FAN // ROWS):
        high, low = split(part_ref[tile])
        out = dot(tab_ref[tile, 0], high) + dot(tab_ref[tile, 0], low) + dot(tab_ref[tile, 1], high)
        half = out.shape[0] // 2
        power = (out[:half] * out[:half] + out[half:] * out[half:]) * scale
        for c in range(channels):
            for m in range(step):
                low_piece = high_piece = None
                for b in range(PACK):
                    d2 = b * step + m
                    x = power[d2 * ROWS : (d2 + 1) * ROWS, c * LANES : (c + 1) * LANES]
                    at = d2 * FAN + tile * ROWS
                    pow_ref[c, at : at + ROWS, :] = x
                    down = pltpu.roll(x, b * PARTS, 1) if b else x
                    shift = (b * PARTS - (LANES - PARTS)) % LANES
                    up = pltpu.roll(x, shift, 1) if shift else x
                    mine = lane >= b * PARTS
                    low_piece = down if low_piece is None else jnp.where(mine, down, low_piece)
                    high_piece = up if high_piece is None else jnp.where(mine, up, high_piece)
                at = c * (PULSES // PACK) + m * FAN + tile * ROWS
                first_ref[at : at + ROWS, :] = jnp.where(even, high_piece, low_piece)
                second_ref[at : at + ROWS, :] = jnp.where(even, low_piece, high_piece)


def doppler(received, channels, limit):
    sets = received.shape[1] // (2 * ROWS)
    vmem = pl.BlockSpec(memory_space=pltpu.VMEM)
    edge = pltpu.VMEM((channels * PULSES // PACK, LANES), F32)
    tables = jnp.asarray(doppler_tables())
    return pl.pallas_call(
        doppler_kernel,
        out_shape=(pltpu.VMEM((channels, PULSES, LANES), F32), edge, edge),
        in_specs=[vmem, vmem],
        out_specs=(vmem, vmem, vmem),
        scratch_shapes=[
            pltpu.VMEM((sets, 2, FAN, ROWS, LANES), F32),
            pltpu.VMEM((FAN // ROWS, 2 * FINE * ROWS, channels * LANES), F32),
        ],
        compiler_params=pltpu.CompilerParams(vmem_limit_bytes=limit),
        cost_estimate=pl.CostEstimate(flops=2 * 10**9, bytes_accessed=2 * MEBI, transcendentals=0),
        name="doppler",
    )(
        pltpu.with_memory_space_constraint(received, pltpu.VMEM),
        pltpu.with_memory_space_constraint(tables, pltpu.VMEM),
    )


def windows_kernel(groups, window_ref, thresh_ref, core_ref, side_ref, line_ref):
    channels = window_ref.shape[0]
    total = groups * LANES
    gate = lax.broadcasted_iota(jnp.int32, (ROWS, LANES), 1) + lax.axis_index("pulse") * LANES
    row_id = lax.broadcasted_iota(jnp.int32, (LANES, LANES), 0)
    col_id = lax.broadcasted_iota(jnp.int32, (LANES, LANES), 1)
    piece, inner = row_id // PARTS, row_id % PARTS
    odd = lax.rem(lax.axis_index("pulse"), 2)
    first = LANES - odd * (LANES + PARTS)
    second = odd * (LANES + PARTS) - PARTS
    core_ref[...] = jnp.zeros_like(core_ref)
    for c in range(channels):
        guard, train = window_ref[c, 0], window_ref[c, 1]
        reach = guard + train

        def band(offset, extra=True):
            distance = jnp.abs(offset)
            return jnp.where((distance > guard) & (distance <= reach) & extra, 1.0, 0.0).astype(BF16)

        core_ref[c * LANES : (c + 1) * LANES, c * LANES : (c + 1) * LANES] = band(row_id - col_id)
        for b in range(PACK):
            at = b * LANES
            side_ref[c, :LANES, at : at + LANES] = band(inner + first - col_id, piece == b)
            side_ref[c, LANES:, at : at + LANES] = band(inner + second - col_id, piece == b)
        ahead = total - 1 - gate
        cells = jnp.minimum(gate, reach) - jnp.minimum(gate, guard)
        cells = cells + jnp.minimum(ahead, reach) - jnp.minimum(ahead, guard)
        line_ref[c, 0] = cells.astype(F32)
        over = jnp.zeros((ROWS, LANES), F32) + thresh_ref[c, 1].astype(F32)
        line_ref[c, 1] = over / thresh_ref[c, 0].astype(F32)


def windows(window, thresh, groups, limit):
    channels = window.shape[0]
    vmem = pl.BlockSpec(memory_space=pltpu.VMEM)
    smem = pl.BlockSpec(memory_space=pltpu.SMEM)
    return pl.pallas_call(
        functools.partial(windows_kernel, groups),
        out_shape=(
            pltpu.VMEM((channels * LANES, channels * LANES), BF16),
            pltpu.VMEM((channels, 2 * LANES, PACK * LANES), BF16),
            pltpu.VMEM((channels, 2, ROWS, LANES), F32),
        ),
        in_specs=[smem, smem],
        out_specs=(vmem, vmem, vmem),
        compiler_params=pltpu.CompilerParams(vmem_limit_bytes=limit),
        cost_estimate=pl.CostEstimate(flops=10**7, bytes_accessed=MEBI, transcendentals=0),
        name="windows",
    )(window, thresh)


def core_kernel(pow_ref, band_ref, noise_ref):
    channels = pow_ref.shape[0]
    high, low = split(jnp.concatenate([pow_ref[c] for c in range(channels)], axis=1))
    noise = dot(high, band_ref[...]) + dot(low, band_ref[...])
    for c in range(channels):
        noise_ref[c] = noise[:, c * LANES : (c + 1) * LANES]


def core(power, band, limit):
    vmem = pl.BlockSpec(memory_space=pltpu.VMEM)
    return pl.pallas_call(
        core_kernel,
        out_shape=pltpu.VMEM(power.shape, F32),
        in_specs=[vmem, vmem],
        out_specs=vmem,
        compiler_params=pltpu.CompilerParams(vmem_limit_bytes=limit),
        cost_estimate=pl.CostEstimate(flops=2 * 10**9, bytes_accessed=MEBI, transcendentals=0),
        name="core",
    )(in_vmem(power), in_vmem(band))


def in_vmem(x):
    return pltpu.with_memory_space_constraint(x, pltpu.VMEM)


def cfar_kernel(pow_ref, noise_ref, first_ref, second_ref, side_ref, line_ref, ratio_ref, out_hbm, soft_ref, sem):
    channels = pow_ref.shape[0]
    rows = PULSES // PACK
    soft_sum = jnp.zeros((ROWS, LANES), F32)
    for c in range(channels):
        halo = jnp.concatenate([ref[c * rows : (c + 1) * rows, :] for ref in (first_ref, second_ref)], axis=1)
        high, low = split(halo)
        side = dot(high, side_ref[c]) + dot(low, side_ref[c])
        cells = jnp.concatenate([line_ref[c, 0]] * (rows // ROWS), axis=0)
        over = jnp.concatenate([line_ref[c, 1]] * (rows // ROWS), axis=0)
        for b in range(PACK):
            at = b * rows
            noise = noise_ref[c, at : at + rows, :] + side[:, b * LANES : (b + 1) * LANES]
            ratio = pow_ref[c, at : at + rows, :] * cells / (noise + EPSILON)
            ratio_ref[c, at : at + rows, :] = ratio
            soft = jnp.clip(ratio * over - 1.0, 0.0, 1.0)
            soft_sum = soft_sum + soft.reshape(rows // ROWS, ROWS, LANES).sum(axis=0)
    count = jnp.sum(soft_sum, axis=0, keepdims=True) * (1024.0 / (PULSES * RANGE))
    soft_ref[...] = jnp.broadcast_to(count, soft_ref.shape)

    @pl.when(stores_early())
    def _():
        store = pltpu.make_async_copy(ratio_ref, out_hbm, sem)
        store.start()
        store.wait()


def stores_early():
    return lax.axis_index("pulse") == 0


def cfar(power, noise, first, second, side, line, peers, limit):
    vmem = pl.BlockSpec(memory_space=pltpu.VMEM)
    return pl.pallas_call(
        cfar_kernel,
        out_shape=(pltpu.VMEM(power.shape, F32), pltpu.HBM(power.shape, F32), pltpu.VMEM((peers, LANES), F32)),
        in_specs=[vmem] * 6,
        out_specs=(vmem, pl.BlockSpec(memory_space=pltpu.HBM), vmem),
        scratch_shapes=[pltpu.SemaphoreType.DMA],
        compiler_params=pltpu.CompilerParams(vmem_limit_bytes=limit),
        cost_estimate=pl.CostEstimate(flops=10**9, bytes_accessed=2 * MEBI, transcendentals=0),
        name="cfar",
    )(*[in_vmem(x) for x in (power, noise, first, second, side, line)])


def finish_kernel(counts_ref, ratio_ref, _, out_hbm, sum_ref, sem):
    store = pltpu.make_async_copy(ratio_ref, out_hbm, sem)
    late = jnp.logical_not(stores_early())

    @pl.when(late)
    def _():
        store.start()

    sum_ref[0] = jnp.sum(counts_ref[...])

    @pl.when(late)
    def _():
        store.wait()


def finish(counts, ratio, partial, limit):
    vmem, hbm = pl.BlockSpec(memory_space=pltpu.VMEM), pl.BlockSpec(memory_space=pltpu.HBM)
    return pl.pallas_call(
        finish_kernel,
        out_shape=(pltpu.HBM(ratio.shape, F32), jax.ShapeDtypeStruct((1,), F32)),
        in_specs=[vmem, vmem, hbm],
        out_specs=(hbm, pl.BlockSpec(memory_space=pltpu.SMEM)),
        scratch_shapes=[pltpu.SemaphoreType.DMA],
        input_output_aliases={2: 0},
        compiler_params=pltpu.CompilerParams(vmem_limit_bytes=limit),
        cost_estimate=pl.CostEstimate(flops=10**5, bytes_accessed=MEBI, transcendentals=0),
        name="finish",
    )(in_vmem(counts), in_vmem(ratio), partial)


def local(samples, replica, window, thresh):
    groups = lax.axis_size("pulse")
    channels = samples.shape[1]
    assert samples.shape[3] == RANGE and groups == FAN and samples.shape[2] == FINE
    limit = 24 * MEBI
    ready = compress(samples, replica, limit)
    received = lax.all_to_all(ready, "pulse", 0, 0, axis_index_groups=[ORDER])
    power, first, second = doppler(received, channels, limit)
    window, first = lax.optimization_barrier((window, first))
    band, side, line = windows(window, thresh, groups, limit)
    first = lax.ppermute(first, "pulse", [(i, i ^ 1) for i in range(groups)])
    second = lax.ppermute(second, "pulse", [(i, ((i + 1) ^ 1) - 1) for i in range(1, groups - 1)])
    noise = core(power, band, limit)
    peers = lax.axis_size("chan") * lax.axis_size("sub")
    ratio, partial, soft = cfar(power, noise, first, second, side, line, peers, limit)
    near = [i ^ (peers // 2 + 1) for i in range(peers)]
    far = [(i + groups // 2) % groups for i in range(groups)]
    soft = soft.reshape(peers, 1, LANES)
    plane = jnp.sum(lax.all_to_all(soft, ("chan", "sub"), 0, 0, axis_index_groups=[near]), axis=0, keepdims=True)
    counts = lax.all_to_all(jnp.broadcast_to(plane, (groups, 1, LANES)), "pulse", 0, 0, axis_index_groups=[far])
    return finish(counts.reshape(groups, LANES), ratio, partial, limit)


def solution(mesh):
    in_specs = (
        P(None, ("grp", "chan", "sub"), "pulse", None),
        P(),
        P(("grp", "chan", "sub"), None),
        P(("grp", "chan", "sub"), None),
    )
    out_specs = (P(("grp", "chan", "sub"), None, "pulse"), P("grp"))
    return jax.shard_map(local, mesh=mesh, in_specs=in_specs, out_specs=out_specs, check_vma=False)
```

```python
import functools
import math

import jax
import jax.numpy as jnp
import numpy as np
from jax import lax
from jax.experimental import pallas as pl
from jax.experimental.pallas import tpu as pltpu
from jax.sharding import PartitionSpec as P

PULSES = 512
RANGE = 4096
GUARD_MAX = 4
TRAIN_MAX = 28

EPSILON = 1e-06
INPUT_SCALE = 1.0 / 2048.0
MARGIN = GUARD_MAX + TRAIN_MAX

LANES = 128
ROWS = 8
FAN = 32
TAIL = RANGE // FAN
FINE = PULSES // FAN
PARTS = MARGIN
PACK = LANES // PARTS
F32 = jnp.float32
BF16 = jnp.bfloat16
MEBI = 1 << 20
ORDER = [0, 1, 31, 2, 6, 7, 5, 12, 4, 13, 10, 14, 15, 9, 11, 24, 8, 25, 27, 26, 30, 28, 29, 3, 20, 21, 23, 22, 18, 19, 17, 16]


def slot(device):
    return ORDER.index(device)


def split_table(table):
    high = table.astype(BF16)
    low = (table - high.astype(np.float64)).astype(BF16)
    return np.stack([high, low])


def unit(product, period):
    angle = 2.0 * np.pi / period * (np.asarray(product, np.int64) % period)
    return np.cos(angle), np.sin(angle)


def range_tables():
    b = np.arange(TAIL)[:, None]
    col = np.arange(TAIL)[None, :]
    freq = 4 * (col % FAN) + col // FAN
    cos, sin = unit(b * freq, TAIL)
    forward = np.block([[cos, -sin], [sin, cos]])
    inverse = forward.T
    k1 = np.arange(FAN)[:, None]
    cos, sin = unit(k1 * np.arange(TAIL)[None, :], RANGE)
    twiddle = np.stack([cos, sin]).astype(np.float32)
    return split_table(forward), split_table(inverse), twiddle


def doppler_tables():
    tiles = []
    for t in range(FAN // ROWS):
        table = np.zeros((2, FINE, ROWS, ROWS, 2, FINE))
        for d1 in range(ROWS):
            bins = 8 * t + d1 + FAN * np.arange(FINE)[:, None]
            cos, sin = unit(bins * np.arange(FINE)[None, :], PULSES)
            table[0, :, d1, d1, 0] = cos
            table[0, :, d1, d1, 1] = sin
            table[1, :, d1, d1, 0] = -sin
            table[1, :, d1, d1, 1] = cos
        tiles.append(split_table(table.reshape(2 * PULSES // 4, 2 * PULSES // 4)))
    return np.stack(tiles)


def add(x, y):
    return (x[0] + y[0], x[1] + y[1])


def sub(x, y):
    return (x[0] - y[0], x[1] - y[1])


def turn(x, sign):
    return (-x[1], x[0]) if sign > 0 else (x[1], -x[0])


def add_turn(x, y, sign):
    if sign > 0:
        return (x[0] - y[1], x[1] + y[0])
    return (x[0] + y[1], x[1] - y[0])


def by_constant(x, index, period, sign):
    index = index % period
    if index == 0:
        return x
    angle = 2.0 * math.pi * index / period
    cos, sin = math.cos(angle), sign * math.sin(angle)
    if 8 * index == period:
        return ((x[0] - x[1]) * cos, (x[0] + x[1]) * cos) if sign > 0 else ((x[0] + x[1]) * cos, (x[1] - x[0]) * cos)
    if 4 * index == period:
        return turn(x, sign)
    return (x[0] * cos - x[1] * sin, x[0] * sin + x[1] * cos)


def fft4(x, sign):
    a, b = add(x[0], x[2]), sub(x[0], x[2])
    c, d = add(x[1], x[3]), sub(x[1], x[3])
    return [add(a, c), add_turn(b, d, sign), sub(a, c), add_turn(b, d, -sign)]


def fft8(x, sign):
    even, odd = fft4(x[0::2], sign), fft4(x[1::2], sign)
    root = math.sqrt(0.5)
    out = [None] * 8
    out[0], out[4] = add(even[0], odd[0]), sub(even[0], odd[0])
    out[2], out[6] = add_turn(even[2], odd[2], sign), add_turn(even[2], odd[2], -sign)
    for k in (1, 3):
        o = odd[k]
        if k == 1:
            w = (o[0] - o[1], o[0] + o[1]) if sign > 0 else (o[0] + o[1], o[1] - o[0])
        else:
            w = (-o[0] - o[1], o[0] - o[1]) if sign > 0 else (o[1] - o[0], -o[0] - o[1])
        w = (w[0] * root, w[1] * root)
        out[k], out[k + 4] = add(even[k], w), sub(even[k], w)
    return out


def fft32(load, keep, fetch, store, sign):
    for n2 in range(8):
        mid = fft4([load(n2 + 8 * n1) for n1 in range(4)], sign)
        for k1 in range(4):
            keep(k1 * 8 + n2, by_constant(mid[k1], n2 * k1, 32, sign))
    for k1 in range(4):
        out = fft8([fetch(k1 * 8 + n2) for n2 in range(8)], sign)
        for k2 in range(8):
            store(k1 + 4 * k2, out[k2])


def split(x):
    high = x.astype(BF16)
    return high, (x - high.astype(F32)).astype(BF16)


def dot(x, y):
    return jnp.dot(x, y, preferred_element_type=F32)


def compress_kernel(
    x_hbm, rep_hbm, fwd_hbm, inv_hbm, twd_hbm, o_ref,
    x_ref, rep_ref, fwd_ref, inv_ref, twd_ref, h_ref, mid_ref, high_ref, low_ref, out_ref, sems,
):
    channels, pulses = x_hbm.shape[1], x_hbm.shape[2]
    sets = [(c, p) for c in range(channels) for p in range(0, pulses, ROWS)]
    loads = [
        pltpu.make_async_copy(x_hbm.at[:, c, pl.ds(p, ROWS)], x_ref.at[i], sems.at[i]) for i, (c, p) in enumerate(sets)
    ]
    n = len(sets)
    load_rep = pltpu.make_async_copy(rep_hbm, rep_ref, sems.at[n])
    load_twd = pltpu.make_async_copy(twd_hbm, twd_ref, sems.at[n + 1])
    load_fwd = pltpu.make_async_copy(fwd_hbm, fwd_ref, sems.at[n + 2])
    load_inv = pltpu.make_async_copy(inv_hbm, inv_ref, sems.at[n + 3])
    for load in [loads[0], load_rep, load_twd, load_fwd, *loads[1:], load_inv]:
        load.start()

    load_rep.wait()
    for part in range(2):
        turned = rep_ref[pl.ds(part, FAN, stride=2), :].T
        h_ref[part] = jnp.concatenate([turned[q * FAN : (q + 1) * FAN] for q in range(4)], axis=1)
    load_twd.wait()

    def row(ref, part, k):
        return jnp.broadcast_to(ref[part, k : k + 1, :], (ROWS, LANES))

    def put(i, k, value):
        at = (i * FAN + k) * ROWS
        for part in range(2):
            high, low = split(value[part])
            high_ref[at : at + ROWS, part * LANES : (part + 1) * LANES] = high
            low_ref[at : at + ROWS, part * LANES : (part + 1) * LANES] = low

    def product(table):
        for t in range(4):
            at = pl.ds(t * 256, 256)
            high = high_ref[at]
            out_ref[at] = dot(high, table[0]) + dot(low_ref[at], table[0]) + dot(high, table[1])

    for i in range(n):
        loads[i].wait()

        def load(a, i=i):
            return tuple(x_ref[i, part, :, a * LANES : (a + 1) * LANES].astype(F32) for part in range(2))

        def keep(j, value, i=i):
            mid_ref[i, 0, j], mid_ref[i, 1, j] = value

        def fetch(j, i=i):
            return (mid_ref[i, 0, j], mid_ref[i, 1, j])

        def twisted(k, value, i=i):
            cos, sin = row(twd_ref, 0, k), row(twd_ref, 1, k)
            put(i, k, (value[0] * cos + value[1] * sin, value[1] * cos - value[0] * sin))

        fft32(load, keep, fetch, twisted, -1)
    load_fwd.wait()
    product(fwd_ref)
    for i in range(n):
        for k in range(FAN):
            at = (i * FAN + k) * ROWS
            re, im = out_ref[at : at + ROWS, :LANES], out_ref[at : at + ROWS, LANES:]
            h_re, h_im = row(h_ref, 0, k), row(h_ref, 1, k)
            put(i, k, (re * h_re - im * h_im, re * h_im + im * h_re))
    load_inv.wait()
    product(inv_ref)
    for i in range(n):

        def keep(j, value, i=i):
            mid_ref[i, 0, j], mid_ref[i, 1, j] = value

        def fetch(j, i=i):
            return (mid_ref[i, 0, j], mid_ref[i, 1, j])

        def untwisted(k, i=i):
            at = (i * FAN + k) * ROWS
            re, im = out_ref[at : at + ROWS, :LANES], out_ref[at : at + ROWS, LANES:]
            cos, sin = row(twd_ref, 0, k), row(twd_ref, 1, k)
            return (re * cos - im * sin, im * cos + re * sin)

        def store(a, value, i=i):
            for part in range(2):
                o_ref[slot(a), i * 2 * ROWS + part * ROWS : i * 2 * ROWS + (part + 1) * ROWS, :] = value[part]

        fft32(untwisted, keep, fetch, store, 1)


def compress(samples, replica, limit):
    fwd, inv, twd = [jnp.asarray(table) for table in range_tables()]
    sets = samples.shape[1] * samples.shape[2] // ROWS
    rep = replica.reshape(2, FAN, LANES).transpose(1, 0, 2).reshape(2 * FAN, LANES)
    any_space = pl.BlockSpec(memory_space=pltpu.HBM)
    return pl.pallas_call(
        compress_kernel,
        out_shape=pltpu.VMEM((FAN, sets * 2 * ROWS, LANES), F32),
        in_specs=[any_space] * 5,
        out_specs=pl.BlockSpec(memory_space=pltpu.VMEM),
        scratch_shapes=[
            pltpu.VMEM((sets, 2, ROWS, RANGE), jnp.int32),
            pltpu.VMEM((2 * FAN, LANES), F32),
            pltpu.VMEM((2, 2 * TAIL, 2 * TAIL), BF16),
            pltpu.VMEM((2, 2 * TAIL, 2 * TAIL), BF16),
            pltpu.VMEM((2, FAN, LANES), F32),
            pltpu.VMEM((2, FAN, LANES), F32),
            pltpu.VMEM((sets, 2, FAN, ROWS, LANES), F32),
            pltpu.VMEM((sets * FAN * ROWS, 2 * LANES), BF16),
            pltpu.VMEM((sets * FAN * ROWS, 2 * LANES), BF16),
            pltpu.VMEM((sets * FAN * ROWS, 2 * LANES), F32),
            pltpu.SemaphoreType.DMA((sets + 4,)),
        ],
        compiler_params=pltpu.CompilerParams(vmem_limit_bytes=limit),
        cost_estimate=pl.CostEstimate(flops=2 * 10**9, bytes_accessed=2 * MEBI, transcendentals=0),
        name="compress",
    )(*[pltpu.with_memory_space_constraint(x, pltpu.HBM) for x in (samples, rep, fwd, inv, twd)])


def doppler_kernel(x_ref, tab_ref, pow_ref, first_ref, second_ref, mid_ref, part_ref):
    channels = pow_ref.shape[0]
    sets = x_ref.shape[1] // (2 * ROWS)
    halves = sets // channels
    for i in range(sets):
        c, half = i // halves, i % halves

        def load(s, i=i):
            return tuple(x_ref[slot(s), i * 2 * ROWS + part * ROWS : i * 2 * ROWS + (part + 1) * ROWS, :] for part in range(2))

        def keep(j, value, i=i):
            mid_ref[i, 0, j], mid_ref[i, 1, j] = value

        def fetch(j, i=i):
            return (mid_ref[i, 0, j], mid_ref[i, 1, j])

        def store(k, value, c=c, half=half):
            tile, d1 = k // ROWS, k % ROWS
            for part in range(2):
                at = (d1 * 2 + part) * FINE + half * ROWS
                part_ref[tile, at : at + ROWS, c * LANES : (c + 1) * LANES] = value[part]

        fft32(load, keep, fetch, store, -1)
    scale = INPUT_SCALE * INPUT_SCALE / (float(RANGE) * float(RANGE) * PULSES)
    lane = lax.broadcasted_iota(jnp.int32, (ROWS, LANES), 1)
    even = lax.broadcast(lax.rem(lax.axis_index("pulse"), 2), (ROWS, LANES)) == 0
    step = FINE // PACK
    for tile in range(FAN // ROWS):
        high, low = split(part_ref[tile])
        out = dot(tab_ref[tile, 0], high) + dot(tab_ref[tile, 0], low) + dot(tab_ref[tile, 1], high)
        half = out.shape[0] // 2
        power = (out[:half] * out[:half] + out[half:] * out[half:]) * scale
        for c in range(channels):
            for m in range(step):
                low_piece = high_piece = None
                for b in range(PACK):
                    d2 = b * step + m
                    x = power[d2 * ROWS : (d2 + 1) * ROWS, c * LANES : (c + 1) * LANES]
                    at = d2 * FAN + tile * ROWS
                    pow_ref[c, at : at + ROWS, :] = x
                    down = pltpu.roll(x, b * PARTS, 1) if b else x
                    shift = (b * PARTS - (LANES - PARTS)) % LANES
                    up = pltpu.roll(x, shift, 1) if shift else x
                    mine = lane >= b * PARTS
                    low_piece = down if low_piece is None else jnp.where(mine, down, low_piece)
                    high_piece = up if high_piece is None else jnp.where(mine, up, high_piece)
                at = c * (PULSES // PACK) + m * FAN + tile * ROWS
                first_ref[at : at + ROWS, :] = jnp.where(even, high_piece, low_piece)
                second_ref[at : at + ROWS, :] = jnp.where(even, low_piece, high_piece)


def doppler(received, channels, limit):
    sets = received.shape[1] // (2 * ROWS)
    vmem = pl.BlockSpec(memory_space=pltpu.VMEM)
    edge = pltpu.VMEM((channels * PULSES // PACK, LANES), F32)
    tables = jnp.asarray(doppler_tables())
    return pl.pallas_call(
        doppler_kernel,
        out_shape=(pltpu.VMEM((channels, PULSES, LANES), F32), edge, edge),
        in_specs=[vmem, vmem],
        out_specs=(vmem, vmem, vmem),
        scratch_shapes=[
            pltpu.VMEM((sets, 2, FAN, ROWS, LANES), F32),
            pltpu.VMEM((FAN // ROWS, 2 * FINE * ROWS, channels * LANES), F32),
        ],
        compiler_params=pltpu.CompilerParams(vmem_limit_bytes=limit),
        cost_estimate=pl.CostEstimate(flops=2 * 10**9, bytes_accessed=2 * MEBI, transcendentals=0),
        name="doppler",
    )(
        pltpu.with_memory_space_constraint(received, pltpu.VMEM),
        pltpu.with_memory_space_constraint(tables, pltpu.VMEM),
    )


def windows_kernel(groups, window_ref, thresh_ref, core_ref, side_ref, line_ref):
    channels = window_ref.shape[0]
    total = groups * LANES
    gate = lax.broadcasted_iota(jnp.int32, (ROWS, LANES), 1) + lax.axis_index("pulse") * LANES
    row_id = lax.broadcasted_iota(jnp.int32, (LANES, LANES), 0)
    col_id = lax.broadcasted_iota(jnp.int32, (LANES, LANES), 1)
    piece, inner = row_id // PARTS, row_id % PARTS
    odd = lax.rem(lax.axis_index("pulse"), 2)
    first = LANES - odd * (LANES + PARTS)
    second = odd * (LANES + PARTS) - PARTS
    core_ref[...] = jnp.zeros_like(core_ref)
    for c in range(channels):
        guard, train = window_ref[c, 0], window_ref[c, 1]
        reach = guard + train

        def band(offset, extra=True):
            distance = jnp.abs(offset)
            return jnp.where((distance > guard) & (distance <= reach) & extra, 1.0, 0.0).astype(BF16)

        core_ref[c * LANES : (c + 1) * LANES, c * LANES : (c + 1) * LANES] = band(row_id - col_id)
        for b in range(PACK):
            at = b * LANES
            side_ref[c, :LANES, at : at + LANES] = band(inner + first - col_id, piece == b)
            side_ref[c, LANES:, at : at + LANES] = band(inner + second - col_id, piece == b)
        ahead = total - 1 - gate
        cells = jnp.minimum(gate, reach) - jnp.minimum(gate, guard)
        cells = cells + jnp.minimum(ahead, reach) - jnp.minimum(ahead, guard)
        line_ref[c, 0] = cells.astype(F32)
        over = jnp.zeros((ROWS, LANES), F32) + thresh_ref[c, 1].astype(F32)
        line_ref[c, 1] = over / thresh_ref[c, 0].astype(F32)


def windows(window, thresh, groups, limit):
    channels = window.shape[0]
    vmem = pl.BlockSpec(memory_space=pltpu.VMEM)
    smem = pl.BlockSpec(memory_space=pltpu.SMEM)
    return pl.pallas_call(
        functools.partial(windows_kernel, groups),
        out_shape=(
            pltpu.VMEM((channels * LANES, channels * LANES), BF16),
            pltpu.VMEM((channels, 2 * LANES, PACK * LANES), BF16),
            pltpu.VMEM((channels, 2, ROWS, LANES), F32),
        ),
        in_specs=[smem, smem],
        out_specs=(vmem, vmem, vmem),
        compiler_params=pltpu.CompilerParams(vmem_limit_bytes=limit),
        cost_estimate=pl.CostEstimate(flops=10**7, bytes_accessed=MEBI, transcendentals=0),
        name="windows",
    )(window, thresh)


def core_kernel(pow_ref, band_ref, noise_ref):
    channels = pow_ref.shape[0]
    high, low = split(jnp.concatenate([pow_ref[c] for c in range(channels)], axis=1))
    noise = dot(high, band_ref[...]) + dot(low, band_ref[...])
    for c in range(channels):
        noise_ref[c] = noise[:, c * LANES : (c + 1) * LANES]


def core(power, band, limit):
    vmem = pl.BlockSpec(memory_space=pltpu.VMEM)
    return pl.pallas_call(
        core_kernel,
        out_shape=pltpu.VMEM(power.shape, F32),
        in_specs=[vmem, vmem],
        out_specs=vmem,
        compiler_params=pltpu.CompilerParams(vmem_limit_bytes=limit),
        cost_estimate=pl.CostEstimate(flops=2 * 10**9, bytes_accessed=MEBI, transcendentals=0),
        name="core",
    )(in_vmem(power), in_vmem(band))


def in_vmem(x):
    return pltpu.with_memory_space_constraint(x, pltpu.VMEM)


def cfar_kernel(pow_ref, noise_ref, first_ref, second_ref, side_ref, line_ref, ratio_ref, out_hbm, soft_ref, sem):
    channels = pow_ref.shape[0]
    rows = PULSES // PACK
    soft_sum = jnp.zeros((ROWS, LANES), F32)
    for c in range(channels):
        halo = jnp.concatenate([ref[c * rows : (c + 1) * rows, :] for ref in (first_ref, second_ref)], axis=1)
        high, low = split(halo)
        side = dot(high, side_ref[c]) + dot(low, side_ref[c])
        cells = jnp.concatenate([line_ref[c, 0]] * (rows // ROWS), axis=0)
        over = jnp.concatenate([line_ref[c, 1]] * (rows // ROWS), axis=0)
        for b in range(PACK):
            at = b * rows
            noise = noise_ref[c, at : at + rows, :] + side[:, b * LANES : (b + 1) * LANES]
            ratio = pow_ref[c, at : at + rows, :] * cells / (noise + EPSILON)
            ratio_ref[c, at : at + rows, :] = ratio
            soft = jnp.clip(ratio * over - 1.0, 0.0, 1.0)
            soft_sum = soft_sum + soft.reshape(rows // ROWS, ROWS, LANES).sum(axis=0)
    count = jnp.sum(soft_sum, axis=0, keepdims=True) * (1024.0 / (PULSES * RANGE))
    soft_ref[...] = jnp.broadcast_to(count, soft_ref.shape)

    @pl.when(stores_early())
    def _():
        store = pltpu.make_async_copy(ratio_ref, out_hbm, sem)
        store.start()
        store.wait()


def stores_early():
    return lax.axis_index("pulse") == 0


def cfar(power, noise, first, second, side, line, peers, limit):
    vmem = pl.BlockSpec(memory_space=pltpu.VMEM)
    return pl.pallas_call(
        cfar_kernel,
        out_shape=(pltpu.VMEM(power.shape, F32), pltpu.HBM(power.shape, F32), pltpu.VMEM((peers, LANES), F32)),
        in_specs=[vmem] * 6,
        out_specs=(vmem, pl.BlockSpec(memory_space=pltpu.HBM), vmem),
        scratch_shapes=[pltpu.SemaphoreType.DMA],
        compiler_params=pltpu.CompilerParams(vmem_limit_bytes=limit),
        cost_estimate=pl.CostEstimate(flops=10**9, bytes_accessed=2 * MEBI, transcendentals=0),
        name="cfar",
    )(*[in_vmem(x) for x in (power, noise, first, second, side, line)])


def finish_kernel(counts_ref, ratio_ref, _, out_hbm, sum_ref, sem):
    store = pltpu.make_async_copy(ratio_ref, out_hbm, sem)
    late = jnp.logical_not(stores_early())

    @pl.when(late)
    def _():
        store.start()

    sum_ref[0] = jnp.sum(counts_ref[...])

    @pl.when(late)
    def _():
        store.wait()


def finish(counts, ratio, partial, limit):
    vmem, hbm = pl.BlockSpec(memory_space=pltpu.VMEM), pl.BlockSpec(memory_space=pltpu.HBM)
    return pl.pallas_call(
        finish_kernel,
        out_shape=(pltpu.HBM(ratio.shape, F32), jax.ShapeDtypeStruct((1,), F32)),
        in_specs=[vmem, vmem, hbm],
        out_specs=(hbm, pl.BlockSpec(memory_space=pltpu.SMEM)),
        scratch_shapes=[pltpu.SemaphoreType.DMA],
        input_output_aliases={2: 0},
        compiler_params=pltpu.CompilerParams(vmem_limit_bytes=limit),
        cost_estimate=pl.CostEstimate(flops=10**5, bytes_accessed=MEBI, transcendentals=0),
        name="finish",
    )(in_vmem(counts), in_vmem(ratio), partial)


def local(samples, replica, window, thresh):
    groups = lax.axis_size("pulse")
    channels = samples.shape[1]
    assert samples.shape[3] == RANGE and groups == FAN and samples.shape[2] == FINE
    limit = 24 * MEBI
    ready = compress(samples, replica, limit)
    received = lax.all_to_all(ready, "pulse", 0, 0, axis_index_groups=[ORDER])
    power, first, second = doppler(received, channels, limit)
    window, first = lax.optimization_barrier((window, first))
    band, side, line = windows(window, thresh, groups, limit)
    first = lax.ppermute(first, "pulse", [(i, i ^ 1) for i in range(groups)])
    second = lax.ppermute(second, "pulse", [(i, ((i + 1) ^ 1) - 1) for i in range(1, groups - 1)])
    noise = core(power, band, limit)
    peers = lax.axis_size("chan") * lax.axis_size("sub")
    ratio, partial, soft = cfar(power, noise, first, second, side, line, peers, limit)
    near = [i ^ (peers // 2 + 1) for i in range(peers)]
    far = [(i + groups // 2) % groups for i in range(groups)]
    soft = soft.reshape(peers, 1, LANES)
    plane = jnp.sum(lax.all_to_all(soft, ("chan", "sub"), 0, 0, axis_index_groups=[near]), axis=0, keepdims=True)
    counts = lax.all_to_all(jnp.broadcast_to(plane, (groups, 1, LANES)), "pulse", 0, 0, axis_index_groups=[far])
    return finish(counts.reshape(groups, LANES), ratio, partial, limit)


def solution(mesh):
    in_specs = (
        P(None, ("grp", "chan", "sub"), "pulse", None),
        P(),
        P(("grp", "chan", "sub"), None),
        P(("grp", "chan", "sub"), None),
    )
    out_specs = (P(("grp", "chan", "sub"), None, "pulse"), P("grp"))
    return jax.shard_map(local, mesh=mesh, in_specs=in_specs, out_specs=out_specs, check_vma=False)
```

```python
import functools
import math

import jax
import jax.numpy as jnp
import numpy as np
from jax import lax
from jax.experimental import pallas as pl
from jax.experimental.pallas import tpu as pltpu
from jax.sharding import PartitionSpec as P

PULSES = 512
RANGE = 4096
GUARD_MAX = 4
TRAIN_MAX = 28

EPSILON = 1e-06
INPUT_SCALE = 1.0 / 2048.0
MARGIN = GUARD_MAX + TRAIN_MAX

LANES = 128
ROWS = 8
FAN = 32
TAIL = RANGE // FAN
FINE = PULSES // FAN
PARTS = MARGIN
PACK = LANES // PARTS
F32 = jnp.float32
BF16 = jnp.bfloat16
MEBI = 1 << 20
ORDER = [0, 1, 31, 2, 6, 7, 5, 12, 4, 13, 10, 14, 15, 9, 11, 24, 8, 25, 27, 26, 30, 29, 28, 3, 20, 21, 23, 22, 18, 19, 17, 16]


def slot(device):
    return ORDER.index(device)


def split_table(table):
    high = table.astype(BF16)
    low = (table - high.astype(np.float64)).astype(BF16)
    return np.stack([high, low])


def unit(product, period):
    angle = 2.0 * np.pi / period * (np.asarray(product, np.int64) % period)
    return np.cos(angle), np.sin(angle)


def range_tables():
    b = np.arange(TAIL)[:, None]
    col = np.arange(TAIL)[None, :]
    freq = 4 * (col % FAN) + col // FAN
    cos, sin = unit(b * freq, TAIL)
    forward = np.block([[cos, -sin], [sin, cos]])
    inverse = forward.T
    k1 = np.arange(FAN)[:, None]
    cos, sin = unit(k1 * np.arange(TAIL)[None, :], RANGE)
    twiddle = np.stack([cos, sin]).astype(np.float32)
    return split_table(forward), split_table(inverse), twiddle


def doppler_tables():
    tiles = []
    for t in range(FAN // ROWS):
        table = np.zeros((2, FINE, ROWS, ROWS, 2, FINE))
        for d1 in range(ROWS):
            bins = 8 * t + d1 + FAN * np.arange(FINE)[:, None]
            cos, sin = unit(bins * np.arange(FINE)[None, :], PULSES)
            table[0, :, d1, d1, 0] = cos
            table[0, :, d1, d1, 1] = sin
            table[1, :, d1, d1, 0] = -sin
            table[1, :, d1, d1, 1] = cos
        tiles.append(split_table(table.reshape(2 * PULSES // 4, 2 * PULSES // 4)))
    return np.stack(tiles)


def add(x, y):
    return (x[0] + y[0], x[1] + y[1])


def sub(x, y):
    return (x[0] - y[0], x[1] - y[1])


def turn(x, sign):
    return (-x[1], x[0]) if sign > 0 else (x[1], -x[0])


def add_turn(x, y, sign):
    if sign > 0:
        return (x[0] - y[1], x[1] + y[0])
    return (x[0] + y[1], x[1] - y[0])


def by_constant(x, index, period, sign):
    index = index % period
    if index == 0:
        return x
    angle = 2.0 * math.pi * index / period
    cos, sin = math.cos(angle), sign * math.sin(angle)
    if 8 * index == period:
        return ((x[0] - x[1]) * cos, (x[0] + x[1]) * cos) if sign > 0 else ((x[0] + x[1]) * cos, (x[1] - x[0]) * cos)
    if 4 * index == period:
        return turn(x, sign)
    return (x[0] * cos - x[1] * sin, x[0] * sin + x[1] * cos)


def fft4(x, sign):
    a, b = add(x[0], x[2]), sub(x[0], x[2])
    c, d = add(x[1], x[3]), sub(x[1], x[3])
    return [add(a, c), add_turn(b, d, sign), sub(a, c), add_turn(b, d, -sign)]


def fft8(x, sign):
    even, odd = fft4(x[0::2], sign), fft4(x[1::2], sign)
    root = math.sqrt(0.5)
    out = [None] * 8
    out[0], out[4] = add(even[0], odd[0]), sub(even[0], odd[0])
    out[2], out[6] = add_turn(even[2], odd[2], sign), add_turn(even[2], odd[2], -sign)
    for k in (1, 3):
        o = odd[k]
        if k == 1:
            w = (o[0] - o[1], o[0] + o[1]) if sign > 0 else (o[0] + o[1], o[1] - o[0])
        else:
            w = (-o[0] - o[1], o[0] - o[1]) if sign > 0 else (o[1] - o[0], -o[0] - o[1])
        w = (w[0] * root, w[1] * root)
        out[k], out[k + 4] = add(even[k], w), sub(even[k], w)
    return out


def fft32(load, keep, fetch, store, sign):
    for n2 in range(8):
        mid = fft4([load(n2 + 8 * n1) for n1 in range(4)], sign)
        for k1 in range(4):
            keep(k1 * 8 + n2, by_constant(mid[k1], n2 * k1, 32, sign))
    for k1 in range(4):
        out = fft8([fetch(k1 * 8 + n2) for n2 in range(8)], sign)
        for k2 in range(8):
            store(k1 + 4 * k2, out[k2])


def split(x):
    high = x.astype(BF16)
    return high, (x - high.astype(F32)).astype(BF16)


def dot(x, y):
    return jnp.dot(x, y, preferred_element_type=F32)


def compress_kernel(
    x_hbm, rep_hbm, fwd_hbm, inv_hbm, twd_hbm, o_ref,
    x_ref, rep_ref, fwd_ref, inv_ref, twd_ref, h_ref, mid_ref, high_ref, low_ref, out_ref, sems,
):
    channels, pulses = x_hbm.shape[1], x_hbm.shape[2]
    sets = [(c, p) for c in range(channels) for p in range(0, pulses, ROWS)]
    loads = [
        pltpu.make_async_copy(x_hbm.at[:, c, pl.ds(p, ROWS)], x_ref.at[i], sems.at[i]) for i, (c, p) in enumerate(sets)
    ]
    n = len(sets)
    load_rep = pltpu.make_async_copy(rep_hbm, rep_ref, sems.at[n])
    load_twd = pltpu.make_async_copy(twd_hbm, twd_ref, sems.at[n + 1])
    load_fwd = pltpu.make_async_copy(fwd_hbm, fwd_ref, sems.at[n + 2])
    load_inv = pltpu.make_async_copy(inv_hbm, inv_ref, sems.at[n + 3])
    for load in [loads[0], load_rep, load_twd, load_fwd, *loads[1:], load_inv]:
        load.start()

    load_rep.wait()
    for part in range(2):
        turned = rep_ref[pl.ds(part, FAN, stride=2), :].T
        h_ref[part] = jnp.concatenate([turned[q * FAN : (q + 1) * FAN] for q in range(4)], axis=1)
    load_twd.wait()

    def row(ref, part, k):
        return jnp.broadcast_to(ref[part, k : k + 1, :], (ROWS, LANES))

    def put(i, k, value):
        at = (i * FAN + k) * ROWS
        for part in range(2):
            high, low = split(value[part])
            high_ref[at : at + ROWS, part * LANES : (part + 1) * LANES] = high
            low_ref[at : at + ROWS, part * LANES : (part + 1) * LANES] = low

    def product(table):
        for t in range(4):
            at = pl.ds(t * 256, 256)
            high = high_ref[at]
            out_ref[at] = dot(high, table[0]) + dot(low_ref[at], table[0]) + dot(high, table[1])

    for i in range(n):
        loads[i].wait()

        def load(a, i=i):
            return tuple(x_ref[i, part, :, a * LANES : (a + 1) * LANES].astype(F32) for part in range(2))

        def keep(j, value, i=i):
            mid_ref[i, 0, j], mid_ref[i, 1, j] = value

        def fetch(j, i=i):
            return (mid_ref[i, 0, j], mid_ref[i, 1, j])

        def twisted(k, value, i=i):
            cos, sin = row(twd_ref, 0, k), row(twd_ref, 1, k)
            put(i, k, (value[0] * cos + value[1] * sin, value[1] * cos - value[0] * sin))

        fft32(load, keep, fetch, twisted, -1)
    load_fwd.wait()
    product(fwd_ref)
    for i in range(n):
        for k in range(FAN):
            at = (i * FAN + k) * ROWS
            re, im = out_ref[at : at + ROWS, :LANES], out_ref[at : at + ROWS, LANES:]
            h_re, h_im = row(h_ref, 0, k), row(h_ref, 1, k)
            put(i, k, (re * h_re - im * h_im, re * h_im + im * h_re))
    load_inv.wait()
    product(inv_ref)
    for i in range(n):

        def keep(j, value, i=i):
            mid_ref[i, 0, j], mid_ref[i, 1, j] = value

        def fetch(j, i=i):
            return (mid_ref[i, 0, j], mid_ref[i, 1, j])

        def untwisted(k, i=i):
            at = (i * FAN + k) * ROWS
            re, im = out_ref[at : at + ROWS, :LANES], out_ref[at : at + ROWS, LANES:]
            cos, sin = row(twd_ref, 0, k), row(twd_ref, 1, k)
            return (re * cos - im * sin, im * cos + re * sin)

        def store(a, value, i=i):
            for part in range(2):
                o_ref[slot(a), i * 2 * ROWS + part * ROWS : i * 2 * ROWS + (part + 1) * ROWS, :] = value[part]

        fft32(untwisted, keep, fetch, store, 1)


def compress(samples, replica, limit):
    fwd, inv, twd = [jnp.asarray(table) for table in range_tables()]
    sets = samples.shape[1] * samples.shape[2] // ROWS
    rep = replica.reshape(2, FAN, LANES).transpose(1, 0, 2).reshape(2 * FAN, LANES)
    any_space = pl.BlockSpec(memory_space=pltpu.HBM)
    return pl.pallas_call(
        compress_kernel,
        out_shape=pltpu.VMEM((FAN, sets * 2 * ROWS, LANES), F32),
        in_specs=[any_space] * 5,
        out_specs=pl.BlockSpec(memory_space=pltpu.VMEM),
        scratch_shapes=[
            pltpu.VMEM((sets, 2, ROWS, RANGE), jnp.int32),
            pltpu.VMEM((2 * FAN, LANES), F32),
            pltpu.VMEM((2, 2 * TAIL, 2 * TAIL), BF16),
            pltpu.VMEM((2, 2 * TAIL, 2 * TAIL), BF16),
            pltpu.VMEM((2, FAN, LANES), F32),
            pltpu.VMEM((2, FAN, LANES), F32),
            pltpu.VMEM((sets, 2, FAN, ROWS, LANES), F32),
            pltpu.VMEM((sets * FAN * ROWS, 2 * LANES), BF16),
            pltpu.VMEM((sets * FAN * ROWS, 2 * LANES), BF16),
            pltpu.VMEM((sets * FAN * ROWS, 2 * LANES), F32),
            pltpu.SemaphoreType.DMA((sets + 4,)),
        ],
        compiler_params=pltpu.CompilerParams(vmem_limit_bytes=limit),
        cost_estimate=pl.CostEstimate(flops=2 * 10**9, bytes_accessed=2 * MEBI, transcendentals=0),
        name="compress",
    )(*[pltpu.with_memory_space_constraint(x, pltpu.HBM) for x in (samples, rep, fwd, inv, twd)])


def doppler_kernel(x_ref, tab_ref, pow_ref, first_ref, second_ref, mid_ref, part_ref):
    channels = pow_ref.shape[0]
    sets = x_ref.shape[1] // (2 * ROWS)
    halves = sets // channels
    for i in range(sets):
        c, half = i // halves, i % halves

        def load(s, i=i):
            return tuple(x_ref[slot(s), i * 2 * ROWS + part * ROWS : i * 2 * ROWS + (part + 1) * ROWS, :] for part in range(2))

        def keep(j, value, i=i):
            mid_ref[i, 0, j], mid_ref[i, 1, j] = value

        def fetch(j, i=i):
            return (mid_ref[i, 0, j], mid_ref[i, 1, j])

        def store(k, value, c=c, half=half):
            tile, d1 = k // ROWS, k % ROWS
            for part in range(2):
                at = (d1 * 2 + part) * FINE + half * ROWS
                part_ref[tile, at : at + ROWS, c * LANES : (c + 1) * LANES] = value[part]

        fft32(load, keep, fetch, store, -1)
    scale = INPUT_SCALE * INPUT_SCALE / (float(RANGE) * float(RANGE) * PULSES)
    lane = lax.broadcasted_iota(jnp.int32, (ROWS, LANES), 1)
    even = lax.broadcast(lax.rem(lax.axis_index("pulse"), 2), (ROWS, LANES)) == 0
    step = FINE // PACK
    for tile in range(FAN // ROWS):
        high, low = split(part_ref[tile])
        out = dot(tab_ref[tile, 0], high) + dot(tab_ref[tile, 0], low) + dot(tab_ref[tile, 1], high)
        half = out.shape[0] // 2
        power = (out[:half] * out[:half] + out[half:] * out[half:]) * scale
        for c in range(channels):
            for m in range(step):
                low_piece = high_piece = None
                for b in range(PACK):
                    d2 = b * step + m
                    x = power[d2 * ROWS : (d2 + 1) * ROWS, c * LANES : (c + 1) * LANES]
                    at = d2 * FAN + tile * ROWS
                    pow_ref[c, at : at + ROWS, :] = x
                    down = pltpu.roll(x, b * PARTS, 1) if b else x
                    shift = (b * PARTS - (LANES - PARTS)) % LANES
                    up = pltpu.roll(x, shift, 1) if shift else x
                    mine = lane >= b * PARTS
                    low_piece = down if low_piece is None else jnp.where(mine, down, low_piece)
                    high_piece = up if high_piece is None else jnp.where(mine, up, high_piece)
                at = c * (PULSES // PACK) + m * FAN + tile * ROWS
                first_ref[at : at + ROWS, :] = jnp.where(even, high_piece, low_piece)
                second_ref[at : at + ROWS, :] = jnp.where(even, low_piece, high_piece)


def doppler(received, channels, limit):
    sets = received.shape[1] // (2 * ROWS)
    vmem = pl.BlockSpec(memory_space=pltpu.VMEM)
    edge = pltpu.VMEM((channels * PULSES // PACK, LANES), F32)
    tables = jnp.asarray(doppler_tables())
    return pl.pallas_call(
        doppler_kernel,
        out_shape=(pltpu.VMEM((channels, PULSES, LANES), F32), edge, edge),
        in_specs=[vmem, vmem],
        out_specs=(vmem, vmem, vmem),
        scratch_shapes=[
            pltpu.VMEM((sets, 2, FAN, ROWS, LANES), F32),
            pltpu.VMEM((FAN // ROWS, 2 * FINE * ROWS, channels * LANES), F32),
        ],
        compiler_params=pltpu.CompilerParams(vmem_limit_bytes=limit),
        cost_estimate=pl.CostEstimate(flops=2 * 10**9, bytes_accessed=2 * MEBI, transcendentals=0),
        name="doppler",
    )(
        pltpu.with_memory_space_constraint(received, pltpu.VMEM),
        pltpu.with_memory_space_constraint(tables, pltpu.VMEM),
    )


def windows_kernel(groups, window_ref, thresh_ref, core_ref, side_ref, line_ref):
    channels = window_ref.shape[0]
    total = groups * LANES
    gate = lax.broadcasted_iota(jnp.int32, (ROWS, LANES), 1) + lax.axis_index("pulse") * LANES
    row_id = lax.broadcasted_iota(jnp.int32, (LANES, LANES), 0)
    col_id = lax.broadcasted_iota(jnp.int32, (LANES, LANES), 1)
    piece, inner = row_id // PARTS, row_id % PARTS
    odd = lax.rem(lax.axis_index("pulse"), 2)
    first = LANES - odd * (LANES + PARTS)
    second = odd * (LANES + PARTS) - PARTS
    core_ref[...] = jnp.zeros_like(core_ref)
    for c in range(channels):
        guard, train = window_ref[c, 0], window_ref[c, 1]
        reach = guard + train

        def band(offset, extra=True):
            distance = jnp.abs(offset)
            return jnp.where((distance > guard) & (distance <= reach) & extra, 1.0, 0.0).astype(BF16)

        core_ref[c * LANES : (c + 1) * LANES, c * LANES : (c + 1) * LANES] = band(row_id - col_id)
        for b in range(PACK):
            at = b * LANES
            side_ref[c, :LANES, at : at + LANES] = band(inner + first - col_id, piece == b)
            side_ref[c, LANES:, at : at + LANES] = band(inner + second - col_id, piece == b)
        ahead = total - 1 - gate
        cells = jnp.minimum(gate, reach) - jnp.minimum(gate, guard)
        cells = cells + jnp.minimum(ahead, reach) - jnp.minimum(ahead, guard)
        line_ref[c, 0] = cells.astype(F32)
        over = jnp.zeros((ROWS, LANES), F32) + thresh_ref[c, 1].astype(F32)
        line_ref[c, 1] = over / thresh_ref[c, 0].astype(F32)


def windows(window, thresh, groups, limit):
    channels = window.shape[0]
    vmem = pl.BlockSpec(memory_space=pltpu.VMEM)
    smem = pl.BlockSpec(memory_space=pltpu.SMEM)
    return pl.pallas_call(
        functools.partial(windows_kernel, groups),
        out_shape=(
            pltpu.VMEM((channels * LANES, channels * LANES), BF16),
            pltpu.VMEM((channels, 2 * LANES, PACK * LANES), BF16),
            pltpu.VMEM((channels, 2, ROWS, LANES), F32),
        ),
        in_specs=[smem, smem],
        out_specs=(vmem, vmem, vmem),
        compiler_params=pltpu.CompilerParams(vmem_limit_bytes=limit),
        cost_estimate=pl.CostEstimate(flops=10**7, bytes_accessed=MEBI, transcendentals=0),
        name="windows",
    )(window, thresh)


def core_kernel(pow_ref, band_ref, noise_ref):
    channels = pow_ref.shape[0]
    high, low = split(jnp.concatenate([pow_ref[c] for c in range(channels)], axis=1))
    noise = dot(high, band_ref[...]) + dot(low, band_ref[...])
    for c in range(channels):
        noise_ref[c] = noise[:, c * LANES : (c + 1) * LANES]


def core(power, band, limit):
    vmem = pl.BlockSpec(memory_space=pltpu.VMEM)
    return pl.pallas_call(
        core_kernel,
        out_shape=pltpu.VMEM(power.shape, F32),
        in_specs=[vmem, vmem],
        out_specs=vmem,
        compiler_params=pltpu.CompilerParams(vmem_limit_bytes=limit),
        cost_estimate=pl.CostEstimate(flops=2 * 10**9, bytes_accessed=MEBI, transcendentals=0),
        name="core",
    )(in_vmem(power), in_vmem(band))


def in_vmem(x):
    return pltpu.with_memory_space_constraint(x, pltpu.VMEM)


def cfar_kernel(pow_ref, noise_ref, first_ref, second_ref, side_ref, line_ref, ratio_ref, out_hbm, soft_ref, sem):
    channels = pow_ref.shape[0]
    rows = PULSES // PACK
    soft_sum = jnp.zeros((ROWS, LANES), F32)
    for c in range(channels):
        halo = jnp.concatenate([ref[c * rows : (c + 1) * rows, :] for ref in (first_ref, second_ref)], axis=1)
        high, low = split(halo)
        side = dot(high, side_ref[c]) + dot(low, side_ref[c])
        cells = jnp.concatenate([line_ref[c, 0]] * (rows // ROWS), axis=0)
        over = jnp.concatenate([line_ref[c, 1]] * (rows // ROWS), axis=0)
        for b in range(PACK):
            at = b * rows
            noise = noise_ref[c, at : at + rows, :] + side[:, b * LANES : (b + 1) * LANES]
            ratio = pow_ref[c, at : at + rows, :] * cells / (noise + EPSILON)
            ratio_ref[c, at : at + rows, :] = ratio
            soft = jnp.clip(ratio * over - 1.0, 0.0, 1.0)
            soft_sum = soft_sum + soft.reshape(rows // ROWS, ROWS, LANES).sum(axis=0)
    count = jnp.sum(soft_sum, axis=0, keepdims=True) * (1024.0 / (PULSES * RANGE))
    soft_ref[...] = jnp.broadcast_to(count, soft_ref.shape)

    @pl.when(stores_early())
    def _():
        store = pltpu.make_async_copy(ratio_ref, out_hbm, sem)
        store.start()
        store.wait()


def stores_early():
    return lax.axis_index("pulse") == 0


def cfar(power, noise, first, second, side, line, peers, limit):
    vmem = pl.BlockSpec(memory_space=pltpu.VMEM)
    return pl.pallas_call(
        cfar_kernel,
        out_shape=(pltpu.VMEM(power.shape, F32), pltpu.HBM(power.shape, F32), pltpu.VMEM((peers, LANES), F32)),
        in_specs=[vmem] * 6,
        out_specs=(vmem, pl.BlockSpec(memory_space=pltpu.HBM), vmem),
        scratch_shapes=[pltpu.SemaphoreType.DMA],
        compiler_params=pltpu.CompilerParams(vmem_limit_bytes=limit),
        cost_estimate=pl.CostEstimate(flops=10**9, bytes_accessed=2 * MEBI, transcendentals=0),
        name="cfar",
    )(*[in_vmem(x) for x in (power, noise, first, second, side, line)])


def finish_kernel(counts_ref, ratio_ref, _, out_hbm, sum_ref, sem):
    store = pltpu.make_async_copy(ratio_ref, out_hbm, sem)
    late = jnp.logical_not(stores_early())

    @pl.when(late)
    def _():
        store.start()

    sum_ref[0] = jnp.sum(counts_ref[...])

    @pl.when(late)
    def _():
        store.wait()


def finish(counts, ratio, partial, limit):
    vmem, hbm = pl.BlockSpec(memory_space=pltpu.VMEM), pl.BlockSpec(memory_space=pltpu.HBM)
    return pl.pallas_call(
        finish_kernel,
        out_shape=(pltpu.HBM(ratio.shape, F32), jax.ShapeDtypeStruct((1,), F32)),
        in_specs=[vmem, vmem, hbm],
        out_specs=(hbm, pl.BlockSpec(memory_space=pltpu.SMEM)),
        scratch_shapes=[pltpu.SemaphoreType.DMA],
        input_output_aliases={2: 0},
        compiler_params=pltpu.CompilerParams(vmem_limit_bytes=limit),
        cost_estimate=pl.CostEstimate(flops=10**5, bytes_accessed=MEBI, transcendentals=0),
        name="finish",
    )(in_vmem(counts), in_vmem(ratio), partial)


def local(samples, replica, window, thresh):
    groups = lax.axis_size("pulse")
    channels = samples.shape[1]
    assert samples.shape[3] == RANGE and groups == FAN and samples.shape[2] == FINE
    limit = 24 * MEBI
    ready = compress(samples, replica, limit)
    received = lax.all_to_all(ready, "pulse", 0, 0, axis_index_groups=[ORDER])
    power, first, second = doppler(received, channels, limit)
    window, first = lax.optimization_barrier((window, first))
    band, side, line = windows(window, thresh, groups, limit)
    first = lax.ppermute(first, "pulse", [(i, i ^ 1) for i in range(groups)])
    second = lax.ppermute(second, "pulse", [(i, ((i + 1) ^ 1) - 1) for i in range(1, groups - 1)])
    noise = core(power, band, limit)
    peers = lax.axis_size("chan") * lax.axis_size("sub")
    ratio, partial, soft = cfar(power, noise, first, second, side, line, peers, limit)
    near = [i ^ (peers // 2 + 1) for i in range(peers)]
    far = [(i + groups // 2) % groups for i in range(groups)]
    soft = soft.reshape(peers, 1, LANES)
    plane = jnp.sum(lax.all_to_all(soft, ("chan", "sub"), 0, 0, axis_index_groups=[near]), axis=0, keepdims=True)
    counts = lax.all_to_all(jnp.broadcast_to(plane, (groups, 1, LANES)), "pulse", 0, 0, axis_index_groups=[far])
    return finish(counts.reshape(groups, LANES), ratio, partial, limit)


def solution(mesh):
    in_specs = (
        P(None, ("grp", "chan", "sub"), "pulse", None),
        P(),
        P(("grp", "chan", "sub"), None),
        P(("grp", "chan", "sub"), None),
    )
    out_specs = (P(("grp", "chan", "sub"), None, "pulse"), P("grp"))
    return jax.shard_map(local, mesh=mesh, in_specs=in_specs, out_specs=out_specs, check_vma=False)
```

```python
import functools
import math

import jax
import jax.numpy as jnp
import numpy as np
from jax import lax
from jax.experimental import pallas as pl
from jax.experimental.pallas import tpu as pltpu
from jax.sharding import PartitionSpec as P

PULSES = 512
RANGE = 4096
GUARD_MAX = 4
TRAIN_MAX = 28

EPSILON = 1e-06
INPUT_SCALE = 1.0 / 2048.0
MARGIN = GUARD_MAX + TRAIN_MAX

LANES = 128
ROWS = 8
FAN = 32
TAIL = RANGE // FAN
FINE = PULSES // FAN
PARTS = MARGIN
PACK = LANES // PARTS
F32 = jnp.float32
BF16 = jnp.bfloat16
MEBI = 1 << 20
ORDER = [0, 1, 31, 2, 6, 7, 5, 12, 4, 13, 10, 14, 15, 9, 11, 24, 8, 25, 27, 26, 30, 29, 28, 3, 20, 21, 23, 22, 18, 19, 17, 16]


def slot(device):
    return ORDER.index(device)


def split_table(table):
    high = table.astype(BF16)
    low = (table - high.astype(np.float64)).astype(BF16)
    return np.stack([high, low])


def unit(product, period):
    angle = 2.0 * np.pi / period * (np.asarray(product, np.int64) % period)
    return np.cos(angle), np.sin(angle)


def range_tables():
    b = np.arange(TAIL)[:, None]
    col = np.arange(TAIL)[None, :]
    freq = 4 * (col % FAN) + col // FAN
    cos, sin = unit(b * freq, TAIL)
    forward = np.block([[cos, -sin], [sin, cos]])
    inverse = forward.T
    k1 = np.arange(FAN)[:, None]
    cos, sin = unit(k1 * np.arange(TAIL)[None, :], RANGE)
    twiddle = np.stack([cos, sin]).astype(np.float32)
    return split_table(forward), split_table(inverse), twiddle


def doppler_tables():
    tiles = []
    for t in range(FAN // ROWS):
        table = np.zeros((2, FINE, ROWS, ROWS, 2, FINE))
        for d1 in range(ROWS):
            bins = 8 * t + d1 + FAN * np.arange(FINE)[:, None]
            cos, sin = unit(bins * np.arange(FINE)[None, :], PULSES)
            table[0, :, d1, d1, 0] = cos
            table[0, :, d1, d1, 1] = sin
            table[1, :, d1, d1, 0] = -sin
            table[1, :, d1, d1, 1] = cos
        tiles.append(split_table(table.reshape(2 * PULSES // 4, 2 * PULSES // 4)))
    return np.stack(tiles)


def add(x, y):
    return (x[0] + y[0], x[1] + y[1])


def sub(x, y):
    return (x[0] - y[0], x[1] - y[1])


def turn(x, sign):
    return (-x[1], x[0]) if sign > 0 else (x[1], -x[0])


def add_turn(x, y, sign):
    if sign > 0:
        return (x[0] - y[1], x[1] + y[0])
    return (x[0] + y[1], x[1] - y[0])


def by_constant(x, index, period, sign):
    index = index % period
    if index == 0:
        return x
    angle = 2.0 * math.pi * index / period
    cos, sin = math.cos(angle), sign * math.sin(angle)
    if 8 * index == period:
        return ((x[0] - x[1]) * cos, (x[0] + x[1]) * cos) if sign > 0 else ((x[0] + x[1]) * cos, (x[1] - x[0]) * cos)
    if 4 * index == period:
        return turn(x, sign)
    return (x[0] * cos - x[1] * sin, x[0] * sin + x[1] * cos)


def fft4(x, sign):
    a, b = add(x[0], x[2]), sub(x[0], x[2])
    c, d = add(x[1], x[3]), sub(x[1], x[3])
    return [add(a, c), add_turn(b, d, sign), sub(a, c), add_turn(b, d, -sign)]


def fft8(x, sign):
    even, odd = fft4(x[0::2], sign), fft4(x[1::2], sign)
    root = math.sqrt(0.5)
    out = [None] * 8
    out[0], out[4] = add(even[0], odd[0]), sub(even[0], odd[0])
    out[2], out[6] = add_turn(even[2], odd[2], sign), add_turn(even[2], odd[2], -sign)
    for k in (1, 3):
        o = odd[k]
        if k == 1:
            w = (o[0] - o[1], o[0] + o[1]) if sign > 0 else (o[0] + o[1], o[1] - o[0])
        else:
            w = (-o[0] - o[1], o[0] - o[1]) if sign > 0 else (o[1] - o[0], -o[0] - o[1])
        w = (w[0] * root, w[1] * root)
        out[k], out[k + 4] = add(even[k], w), sub(even[k], w)
    return out


def fft32(load, keep, fetch, store, sign):
    for n2 in range(8):
        mid = fft4([load(n2 + 8 * n1) for n1 in range(4)], sign)
        for k1 in range(4):
            keep(k1 * 8 + n2, by_constant(mid[k1], n2 * k1, 32, sign))
    for k1 in range(4):
        out = fft8([fetch(k1 * 8 + n2) for n2 in range(8)], sign)
        for k2 in range(8):
            store(k1 + 4 * k2, out[k2])


def split(x):
    high = x.astype(BF16)
    return high, (x - high.astype(F32)).astype(BF16)


def dot(x, y):
    return jnp.dot(x, y, preferred_element_type=F32)


def compress_kernel(
    x_hbm, rep_hbm, fwd_hbm, inv_hbm, twd_hbm, o_ref,
    x_ref, rep_ref, fwd_ref, inv_ref, twd_ref, h_ref, mid_ref, high_ref, low_ref, out_ref, sems,
):
    channels, pulses = x_hbm.shape[1], x_hbm.shape[2]
    sets = [(c, p) for c in range(channels) for p in range(0, pulses, ROWS)]
    loads = [
        pltpu.make_async_copy(x_hbm.at[:, c, pl.ds(p, ROWS)], x_ref.at[i], sems.at[i]) for i, (c, p) in enumerate(sets)
    ]
    n = len(sets)
    load_rep = pltpu.make_async_copy(rep_hbm, rep_ref, sems.at[n])
    load_twd = pltpu.make_async_copy(twd_hbm, twd_ref, sems.at[n + 1])
    load_fwd = pltpu.make_async_copy(fwd_hbm, fwd_ref, sems.at[n + 2])
    load_inv = pltpu.make_async_copy(inv_hbm, inv_ref, sems.at[n + 3])
    for load in [load_rep, loads[0], load_twd, *loads[1:], load_fwd, load_inv]:
        load.start()

    load_rep.wait()
    for part in range(2):
        turned = rep_ref[pl.ds(part, FAN, stride=2), :].T
        h_ref[part] = jnp.concatenate([turned[q * FAN : (q + 1) * FAN] for q in range(4)], axis=1)
    load_twd.wait()

    def row(ref, part, k):
        return jnp.broadcast_to(ref[part, k : k + 1, :], (ROWS, LANES))

    def put(i, k, value):
        at = (i * FAN + k) * ROWS
        for part in range(2):
            high, low = split(value[part])
            high_ref[at : at + ROWS, part * LANES : (part + 1) * LANES] = high
            low_ref[at : at + ROWS, part * LANES : (part + 1) * LANES] = low

    def product(table):
        for t in range(4):
            at = pl.ds(t * 256, 256)
            high = high_ref[at]
            out_ref[at] = dot(high, table[0]) + dot(low_ref[at], table[0]) + dot(high, table[1])

    for i in range(n):
        loads[i].wait()

        def load(a, i=i):
            return tuple(x_ref[i, part, :, a * LANES : (a + 1) * LANES].astype(F32) for part in range(2))

        def keep(j, value, i=i):
            mid_ref[i, 0, j], mid_ref[i, 1, j] = value

        def fetch(j, i=i):
            return (mid_ref[i, 0, j], mid_ref[i, 1, j])

        def twisted(k, value, i=i):
            cos, sin = row(twd_ref, 0, k), row(twd_ref, 1, k)
            put(i, k, (value[0] * cos + value[1] * sin, value[1] * cos - value[0] * sin))

        fft32(load, keep, fetch, twisted, -1)
    load_fwd.wait()
    product(fwd_ref)
    for i in range(n):
        for k in range(FAN):
            at = (i * FAN + k) * ROWS
            re, im = out_ref[at : at + ROWS, :LANES], out_ref[at : at + ROWS, LANES:]
            h_re, h_im = row(h_ref, 0, k), row(h_ref, 1, k)
            put(i, k, (re * h_re - im * h_im, re * h_im + im * h_re))
    load_inv.wait()
    product(inv_ref)
    for i in range(n):

        def keep(j, value, i=i):
            mid_ref[i, 0, j], mid_ref[i, 1, j] = value

        def fetch(j, i=i):
            return (mid_ref[i, 0, j], mid_ref[i, 1, j])

        def untwisted(k, i=i):
            at = (i * FAN + k) * ROWS
            re, im = out_ref[at : at + ROWS, :LANES], out_ref[at : at + ROWS, LANES:]
            cos, sin = row(twd_ref, 0, k), row(twd_ref, 1, k)
            return (re * cos - im * sin, im * cos + re * sin)

        def store(a, value, i=i):
            for part in range(2):
                o_ref[slot(a), i * 2 * ROWS + part * ROWS : i * 2 * ROWS + (part + 1) * ROWS, :] = value[part]

        fft32(untwisted, keep, fetch, store, 1)


def compress(samples, replica, limit):
    fwd, inv, twd = [jnp.asarray(table) for table in range_tables()]
    sets = samples.shape[1] * samples.shape[2] // ROWS
    rep = replica.reshape(2, FAN, LANES).transpose(1, 0, 2).reshape(2 * FAN, LANES)
    any_space = pl.BlockSpec(memory_space=pltpu.HBM)
    return pl.pallas_call(
        compress_kernel,
        out_shape=pltpu.VMEM((FAN, sets * 2 * ROWS, LANES), F32),
        in_specs=[any_space] * 5,
        out_specs=pl.BlockSpec(memory_space=pltpu.VMEM),
        scratch_shapes=[
            pltpu.VMEM((sets, 2, ROWS, RANGE), jnp.int32),
            pltpu.VMEM((2 * FAN, LANES), F32),
            pltpu.VMEM((2, 2 * TAIL, 2 * TAIL), BF16),
            pltpu.VMEM((2, 2 * TAIL, 2 * TAIL), BF16),
            pltpu.VMEM((2, FAN, LANES), F32),
            pltpu.VMEM((2, FAN, LANES), F32),
            pltpu.VMEM((sets, 2, FAN, ROWS, LANES), F32),
            pltpu.VMEM((sets * FAN * ROWS, 2 * LANES), BF16),
            pltpu.VMEM((sets * FAN * ROWS, 2 * LANES), BF16),
            pltpu.VMEM((sets * FAN * ROWS, 2 * LANES), F32),
            pltpu.SemaphoreType.DMA((sets + 4,)),
        ],
        compiler_params=pltpu.CompilerParams(vmem_limit_bytes=limit),
        cost_estimate=pl.CostEstimate(flops=2 * 10**9, bytes_accessed=2 * MEBI, transcendentals=0),
        name="compress",
    )(*[pltpu.with_memory_space_constraint(x, pltpu.HBM) for x in (samples, rep, fwd, inv, twd)])


def doppler_kernel(x_ref, tab_ref, pow_ref, first_ref, second_ref, mid_ref, part_ref):
    channels = pow_ref.shape[0]
    sets = x_ref.shape[1] // (2 * ROWS)
    halves = sets // channels
    for i in range(sets):
        c, half = i // halves, i % halves

        def load(s, i=i):
            return tuple(x_ref[slot(s), i * 2 * ROWS + part * ROWS : i * 2 * ROWS + (part + 1) * ROWS, :] for part in range(2))

        def keep(j, value, i=i):
            mid_ref[i, 0, j], mid_ref[i, 1, j] = value

        def fetch(j, i=i):
            return (mid_ref[i, 0, j], mid_ref[i, 1, j])

        def store(k, value, c=c, half=half):
            tile, d1 = k // ROWS, k % ROWS
            for part in range(2):
                at = (d1 * 2 + part) * FINE + half * ROWS
                part_ref[tile, at : at + ROWS, c * LANES : (c + 1) * LANES] = value[part]

        fft32(load, keep, fetch, store, -1)
    scale = INPUT_SCALE * INPUT_SCALE / (float(RANGE) * float(RANGE) * PULSES)
    lane = lax.broadcasted_iota(jnp.int32, (ROWS, LANES), 1)
    even = lax.broadcast(lax.rem(lax.axis_index("pulse"), 2), (ROWS, LANES)) == 0
    step = FINE // PACK
    for tile in range(FAN // ROWS):
        high, low = split(part_ref[tile])
        out = dot(tab_ref[tile, 0], high) + dot(tab_ref[tile, 0], low) + dot(tab_ref[tile, 1], high)
        half = out.shape[0] // 2
        power = (out[:half] * out[:half] + out[half:] * out[half:]) * scale
        for c in range(channels):
            for m in range(step):
                low_piece = high_piece = None
                for b in range(PACK):
                    d2 = b * step + m
                    x = power[d2 * ROWS : (d2 + 1) * ROWS, c * LANES : (c + 1) * LANES]
                    at = d2 * FAN + tile * ROWS
                    pow_ref[c, at : at + ROWS, :] = x
                    down = pltpu.roll(x, b * PARTS, 1) if b else x
                    shift = (b * PARTS - (LANES - PARTS)) % LANES
                    up = pltpu.roll(x, shift, 1) if shift else x
                    mine = lane >= b * PARTS
                    low_piece = down if low_piece is None else jnp.where(mine, down, low_piece)
                    high_piece = up if high_piece is None else jnp.where(mine, up, high_piece)
                at = c * (PULSES // PACK) + m * FAN + tile * ROWS
                first_ref[at : at + ROWS, :] = jnp.where(even, high_piece, low_piece)
                second_ref[at : at + ROWS, :] = jnp.where(even, low_piece, high_piece)


def doppler(received, channels, limit):
    sets = received.shape[1] // (2 * ROWS)
    vmem = pl.BlockSpec(memory_space=pltpu.VMEM)
    edge = pltpu.VMEM((channels * PULSES // PACK, LANES), F32)
    tables = jnp.asarray(doppler_tables())
    return pl.pallas_call(
        doppler_kernel,
        out_shape=(pltpu.VMEM((channels, PULSES, LANES), F32), edge, edge),
        in_specs=[vmem, vmem],
        out_specs=(vmem, vmem, vmem),
        scratch_shapes=[
            pltpu.VMEM((sets, 2, FAN, ROWS, LANES), F32),
            pltpu.VMEM((FAN // ROWS, 2 * FINE * ROWS, channels * LANES), F32),
        ],
        compiler_params=pltpu.CompilerParams(vmem_limit_bytes=limit),
        cost_estimate=pl.CostEstimate(flops=2 * 10**9, bytes_accessed=2 * MEBI, transcendentals=0),
        name="doppler",
    )(
        pltpu.with_memory_space_constraint(received, pltpu.VMEM),
        pltpu.with_memory_space_constraint(tables, pltpu.VMEM),
    )


def windows_kernel(groups, window_ref, thresh_ref, core_ref, side_ref, line_ref):
    channels = window_ref.shape[0]
    total = groups * LANES
    gate = lax.broadcasted_iota(jnp.int32, (ROWS, LANES), 1) + lax.axis_index("pulse") * LANES
    row_id = lax.broadcasted_iota(jnp.int32, (LANES, LANES), 0)
    col_id = lax.broadcasted_iota(jnp.int32, (LANES, LANES), 1)
    piece, inner = row_id // PARTS, row_id % PARTS
    odd = lax.rem(lax.axis_index("pulse"), 2)
    first = LANES - odd * (LANES + PARTS)
    second = odd * (LANES + PARTS) - PARTS
    core_ref[...] = jnp.zeros_like(core_ref)
    for c in range(channels):
        guard, train = window_ref[c, 0], window_ref[c, 1]
        reach = guard + train

        def band(offset, extra=True):
            distance = jnp.abs(offset)
            return jnp.where((distance > guard) & (distance <= reach) & extra, 1.0, 0.0).astype(BF16)

        core_ref[c * LANES : (c + 1) * LANES, c * LANES : (c + 1) * LANES] = band(row_id - col_id)
        for b in range(PACK):
            at = b * LANES
            side_ref[c, :LANES, at : at + LANES] = band(inner + first - col_id, piece == b)
            side_ref[c, LANES:, at : at + LANES] = band(inner + second - col_id, piece == b)
        ahead = total - 1 - gate
        cells = jnp.minimum(gate, reach) - jnp.minimum(gate, guard)
        cells = cells + jnp.minimum(ahead, reach) - jnp.minimum(ahead, guard)
        line_ref[c, 0] = cells.astype(F32)
        over = jnp.zeros((ROWS, LANES), F32) + thresh_ref[c, 1].astype(F32)
        line_ref[c, 1] = over / thresh_ref[c, 0].astype(F32)


def windows(window, thresh, groups, limit):
    channels = window.shape[0]
    vmem = pl.BlockSpec(memory_space=pltpu.VMEM)
    smem = pl.BlockSpec(memory_space=pltpu.SMEM)
    return pl.pallas_call(
        functools.partial(windows_kernel, groups),
        out_shape=(
            pltpu.VMEM((channels * LANES, channels * LANES), BF16),
            pltpu.VMEM((channels, 2 * LANES, PACK * LANES), BF16),
            pltpu.VMEM((channels, 2, ROWS, LANES), F32),
        ),
        in_specs=[smem, smem],
        out_specs=(vmem, vmem, vmem),
        compiler_params=pltpu.CompilerParams(vmem_limit_bytes=limit),
        cost_estimate=pl.CostEstimate(flops=10**7, bytes_accessed=MEBI, transcendentals=0),
        name="windows",
    )(window, thresh)


def core_kernel(pow_ref, band_ref, noise_ref):
    channels = pow_ref.shape[0]
    high, low = split(jnp.concatenate([pow_ref[c] for c in range(channels)], axis=1))
    noise = dot(high, band_ref[...]) + dot(low, band_ref[...])
    for c in range(channels):
        noise_ref[c] = noise[:, c * LANES : (c + 1) * LANES]


def core(power, band, limit):
    vmem = pl.BlockSpec(memory_space=pltpu.VMEM)
    return pl.pallas_call(
        core_kernel,
        out_shape=pltpu.VMEM(power.shape, F32),
        in_specs=[vmem, vmem],
        out_specs=vmem,
        compiler_params=pltpu.CompilerParams(vmem_limit_bytes=limit),
        cost_estimate=pl.CostEstimate(flops=2 * 10**9, bytes_accessed=MEBI, transcendentals=0),
        name="core",
    )(in_vmem(power), in_vmem(band))


def in_vmem(x):
    return pltpu.with_memory_space_constraint(x, pltpu.VMEM)


def cfar_kernel(pow_ref, noise_ref, first_ref, second_ref, side_ref, line_ref, ratio_ref, out_hbm, soft_ref, sem):
    channels = pow_ref.shape[0]
    rows = PULSES // PACK
    soft_sum = jnp.zeros((ROWS, LANES), F32)
    for c in range(channels):
        halo = jnp.concatenate([ref[c * rows : (c + 1) * rows, :] for ref in (first_ref, second_ref)], axis=1)
        high, low = split(halo)
        side = dot(high, side_ref[c]) + dot(low, side_ref[c])
        cells = jnp.concatenate([line_ref[c, 0]] * (rows // ROWS), axis=0)
        over = jnp.concatenate([line_ref[c, 1]] * (rows // ROWS), axis=0)
        for b in range(PACK):
            at = b * rows
            noise = noise_ref[c, at : at + rows, :] + side[:, b * LANES : (b + 1) * LANES]
            ratio = pow_ref[c, at : at + rows, :] * cells / (noise + EPSILON)
            ratio_ref[c, at : at + rows, :] = ratio
            soft = jnp.clip(ratio * over - 1.0, 0.0, 1.0)
            soft_sum = soft_sum + soft.reshape(rows // ROWS, ROWS, LANES).sum(axis=0)
    count = jnp.sum(soft_sum, axis=0, keepdims=True) * (1024.0 / (PULSES * RANGE))
    soft_ref[...] = jnp.broadcast_to(count, soft_ref.shape)

    @pl.when(stores_early())
    def _():
        store = pltpu.make_async_copy(ratio_ref, out_hbm, sem)
        store.start()
        store.wait()


def stores_early():
    return lax.axis_index("pulse") == 0


def cfar(power, noise, first, second, side, line, peers, limit):
    vmem = pl.BlockSpec(memory_space=pltpu.VMEM)
    return pl.pallas_call(
        cfar_kernel,
        out_shape=(pltpu.VMEM(power.shape, F32), pltpu.HBM(power.shape, F32), pltpu.VMEM((peers, LANES), F32)),
        in_specs=[vmem] * 6,
        out_specs=(vmem, pl.BlockSpec(memory_space=pltpu.HBM), vmem),
        scratch_shapes=[pltpu.SemaphoreType.DMA],
        compiler_params=pltpu.CompilerParams(vmem_limit_bytes=limit),
        cost_estimate=pl.CostEstimate(flops=10**9, bytes_accessed=2 * MEBI, transcendentals=0),
        name="cfar",
    )(*[in_vmem(x) for x in (power, noise, first, second, side, line)])


def finish_kernel(counts_ref, ratio_ref, _, out_hbm, sum_ref, sem):
    store = pltpu.make_async_copy(ratio_ref, out_hbm, sem)
    late = jnp.logical_not(stores_early())

    @pl.when(late)
    def _():
        store.start()

    sum_ref[0] = jnp.sum(counts_ref[...])

    @pl.when(late)
    def _():
        store.wait()


def finish(counts, ratio, partial, limit):
    vmem, hbm = pl.BlockSpec(memory_space=pltpu.VMEM), pl.BlockSpec(memory_space=pltpu.HBM)
    return pl.pallas_call(
        finish_kernel,
        out_shape=(pltpu.HBM(ratio.shape, F32), jax.ShapeDtypeStruct((1,), F32)),
        in_specs=[vmem, vmem, hbm],
        out_specs=(hbm, pl.BlockSpec(memory_space=pltpu.SMEM)),
        scratch_shapes=[pltpu.SemaphoreType.DMA],
        input_output_aliases={2: 0},
        compiler_params=pltpu.CompilerParams(vmem_limit_bytes=limit),
        cost_estimate=pl.CostEstimate(flops=10**5, bytes_accessed=MEBI, transcendentals=0),
        name="finish",
    )(in_vmem(counts), in_vmem(ratio), partial)


def local(samples, replica, window, thresh):
    groups = lax.axis_size("pulse")
    channels = samples.shape[1]
    assert samples.shape[3] == RANGE and groups == FAN and samples.shape[2] == FINE
    limit = 24 * MEBI
    ready = compress(samples, replica, limit)
    received = lax.all_to_all(ready, "pulse", 0, 0, axis_index_groups=[ORDER])
    power, first, second = doppler(received, channels, limit)
    window, first = lax.optimization_barrier((window, first))
    band, side, line = windows(window, thresh, groups, limit)
    first = lax.ppermute(first, "pulse", [(i, i ^ 1) for i in range(groups)])
    second = lax.ppermute(second, "pulse", [(i, ((i + 1) ^ 1) - 1) for i in range(1, groups - 1)])
    noise = core(power, band, limit)
    peers = lax.axis_size("chan") * lax.axis_size("sub")
    ratio, partial, soft = cfar(power, noise, first, second, side, line, peers, limit)
    near = [i ^ (peers // 2 + 1) for i in range(peers)]
    far = [(i + groups // 2) % groups for i in range(groups)]
    soft = soft.reshape(peers, 1, LANES)
    plane = jnp.sum(lax.all_to_all(soft, ("chan", "sub"), 0, 0, axis_index_groups=[near]), axis=0, keepdims=True)
    counts = lax.all_to_all(jnp.broadcast_to(plane, (groups, 1, LANES)), "pulse", 0, 0, axis_index_groups=[far])
    return finish(counts.reshape(groups, LANES), ratio, partial, limit)


def solution(mesh):
    in_specs = (
        P(None, ("grp", "chan", "sub"), "pulse", None),
        P(),
        P(("grp", "chan", "sub"), None),
        P(("grp", "chan", "sub"), None),
    )
    out_specs = (P(("grp", "chan", "sub"), None, "pulse"), P("grp"))
    return jax.shard_map(local, mesh=mesh, in_specs=in_specs, out_specs=out_specs, check_vma=False)
```
